256 devices in a mesh: dp: 128 (over z, y, x), mp: 2 (over core).
Axes of the slice: x: 4, y: 4, z: 8, core: 2. Of those that a mesh axis runs over, the one named last changes fastest.
Arguments:
- points: bfloat16 [131072, 1024], P(('dp', 'mp')), may hold values from -6 to 6
- centroids: bfloat16 [4096, 1024], P('mp'), may hold values from -6 to 6
- assign: int32 [131072], P(('dp', 'mp')), may hold values from 0 to 4095
- keep_mask: int32 [131072], P(('dp', 'mp')), may hold values 0 or 1
Outputs:
- new_centroids: float32 [4096, 1024], P('mp')
- row_cost: float32 [131072], P(('dp', 'mp'))
The draws below stay inside these ranges and needn't reach their ends.
All inputs are finite; a program needn't handle non-finite values. No bound on the sum of `keep_mask` on one device may be relied on, other than what follows from the above.
Results may differ from the reference program's by a relative error of at most 0.0008.
Values may be sent and summed in bfloat16 or wider, within the bound.
A program may use at most 128 MiB of HBM per device.

```python
import math
import jax
import jax.numpy as jnp
import numpy as np
from jax import lax

D = 1024
K = 4096
ROWS = 131072


def place_ends(values, stream_key, smallest, high):
    longest = values.shape.index(max(values.shape))
    spots = []
    for shift in (0, 1):
        where = [jax.random.randint(jax.random.fold_in(stream_key, axis), (), 0, length) for axis, length in enumerate(values.shape)]
        where[longest] = (where[longest] + shift) % values.shape[longest]
        spots.append(tuple(where))
    return values.at[spots[0]].set(smallest).at[spots[1]].set(high)


def block_scale(own_key, dims, shards, smallest, high):
    level = 1.0
    for axis_at, shards_of in shards:
        draws = jax.random.uniform(jax.random.fold_in(jax.random.fold_in(own_key, 6), axis_at), (shards_of,), jnp.float32, smallest / len(shards), high / len(shards))
        level = level * jnp.repeat(jnp.exp(draws), dims[axis_at] // shards_of).reshape((-1,) + (1,) * (len(dims) - 1 - axis_at))
    return level


def cumulative_ranks(count, lean):
    portions = [(1 << 20) // math.isqrt(standing ** lean) + 1 for standing in range(1, count + 1)]
    width = 1 + sum(portions) // (1 << 30)
    return np.cumsum(np.array([max(1, weight // width) for weight in portions]))


def skewed_ids(own_key, extent, count, skew):
    grid = cumulative_ranks(count, skew)
    pick = jax.random.randint(jax.random.fold_in(own_key, 1), extent, 0, int(grid[count - 1]))
    standing = jnp.searchsorted(jnp.asarray(grid, jnp.int32), pick, side="right")
    return jax.random.permutation(jax.random.fold_in(own_key, 2), count)[standing].astype(jnp.int32)


def centred(own_key, shape, deviation, limit, cuts=(), kind=jnp.bfloat16):
    result = deviation * jax.random.normal(own_key, shape, jnp.float32)
    if cuts:
        result = result * block_scale(own_key, shape, cuts, -0.22, 0.18)
    return jnp.clip(result, -limit, limit).astype(kind)


def setup_inputs(seed: int = 0) -> dict:
    seeds = jax.random.split(jax.random.key(seed), 5)
    points = centred(seeds[0], (ROWS, D), 1.0, 6.0, ((0, 256),))
    centroids = centred(seeds[1], (K, D), 1.0, 6.0, ((0, 2),))
    assign = place_ends(skewed_ids(seeds[2], (ROWS,), K, 2), jax.random.fold_in(seeds[2], 3), 0, K - 1).astype(jnp.int32)
    keep_mask = place_ends((jax.random.randint(seeds[3], (ROWS,), 0, 4) < 3).astype(jnp.int32), jax.random.fold_in(seeds[3], 1), 0, 1)
    return dict(points=points, centroids=centroids, assign=assign, keep_mask=keep_mask)


def reference(points, centroids, assign, keep_mask):
    cent_f = centroids.astype(jnp.float32)
    cent_sq = jnp.sum(cent_f * cent_f, axis=1)
    block = math.gcd(ROWS, 1024)
    blocks = points.reshape(ROWS // block, block, D)

    def cost_block(group_rows):
        point_f = group_rows.astype(jnp.float32)
        point_sq = jnp.sum(point_f * point_f, axis=1)
        inner = jnp.dot(group_rows, centroids.T, preferred_element_type=jnp.float32)
        dist = point_sq[:, None] - 2.0 * inner + cent_sq[None, :]
        return jnp.min(dist, axis=1) / D

    row_cost = lax.map(cost_block, blocks).reshape(ROWS)
    weights = keep_mask.astype(jnp.float32)
    sums = jax.ops.segment_sum(points.astype(jnp.float32) * weights[:, None], assign, num_segments=K)
    counts = jax.ops.segment_sum(weights, assign, num_segments=K)
    fresh = sums / jnp.maximum(counts, 1.0)[:, None]
    new_centroids = jnp.where(counts[:, None] > 0.5, fresh, cent_f)
    return new_centroids, row_cost
```

```python
import jax
import jax.numpy as jnp
from jax import lax
from jax.experimental import pallas as pl
from jax.experimental.pallas import tpu as pltpu
from jax.sharding import Mesh
from jax.sharding import PartitionSpec as P

STEPS = 32000.0
TINY = 2.0**-100
NX, NY, NZ = 4, 4, 8
LANES = 128
FEATS = 256
CROWS = 512
OWN = 64
TILE = 256
MESH_ID = pl.DeviceIdType.MESH


def encode(v):
    top = jnp.maximum(jnp.max(jnp.abs(v), axis=1, keepdims=True), TINY)
    code = jnp.floor(v * (STEPS / top) + 0.5).astype(jnp.int32)
    return (code[:, :LANES] << 16) | (code[:, LANES:] & 0xFFFF), top * (1.0 / STEPS)


def decode(words, step):
    high = (words >> 16).astype(jnp.float32)
    low = ((words << 16) >> 16).astype(jnp.float32)
    return high * step, low * step


def lane_eye(rows, shift=0):
    at_row = lax.broadcasted_iota(jnp.int32, (rows, LANES), 0)
    at_lane = lax.broadcasted_iota(jnp.int32, (rows, LANES), 1)
    return at_lane == at_row + shift


def to_row(col, eye):
    return jnp.sum(jnp.where(eye, col, 0.0), axis=0, keepdims=True)


def to_col(row, eye):
    return jnp.sum(jnp.where(eye, row, 0.0), axis=1, keepdims=True)


def update_kernel(
    p_hbm, c_hbm, assign_ref, keep_ref, words_ref, steps_ref, cost_ref,
    pv, cv, near, ids, relay, best, acc, cnt,
    ysend, yaux, yrecv, yauxr, zsend, zaux, zrecv, zauxr,
    send_sem, recv_sem, local_sem,
):
    z, y, x, m = (lax.axis_index(n) for n in ("z", "y", "x", "mp"))
    xr, xl, xo = (lax.rem(x + d, NX) for d in (1, 3, 2))
    yr, yl, yo = (lax.rem(y + d, NY) for d in (1, 3, 2))
    zat = lambda d: lax.rem(z + d + NZ, NZ)
    other = 1 - m
    used = []

    def remote(src, dst, device):
        k = len(used)
        copy = pltpu.make_async_remote_copy(
            src_ref=src, dst_ref=dst, send_sem=send_sem.at[k], recv_sem=recv_sem.at[k],
            device_id=device, device_id_type=MESH_ID,
        )
        copy.start()
        used.append(copy)
        return copy

    at_x = lambda to: (z, y, to, m)
    at_y = lambda to: (z, to, x, m)
    at_z = lambda to: (to, y, x, m)
    partner = (z, y, x, other)

    load_p = pltpu.make_async_copy(p_hbm, pv, local_sem.at[0])
    load_p.start()
    load_c = pltpu.make_async_copy(c_hbm, cv.at[0], local_sem.at[1])
    load_c.start()

    peers = [at_x(xr), at_x(xl), at_x(xo), at_y(yr), at_y(yl), at_y(yo), partner]
    peers += [at_z(zat(d)) for d in range(1, NZ)]
    barrier = pltpu.get_barrier_semaphore()
    for peer in peers:
        pl.semaphore_signal(barrier, inc=1, device_id=peer, device_id_type=MESH_ID)
    pl.semaphore_wait(barrier, len(peers))

    def slot(s):
        return pl.ds(s * 512, 512)

    def cols(f):
        return pl.ds(pl.multiple_of(f * FEATS, FEATS), FEATS)

    ids[:, slot(0)] = jnp.where(keep_ref[...] > 0, assign_ref[...], -1)
    load_p.wait()
    lo, hi = pl.ds(0, 256), pl.ds(256, 256)
    relay_l = remote(pv.at[lo, cols(xo)], relay.at[0], at_x(xr))
    relay_r = remote(pv.at[hi, cols(xo)], relay.at[1], at_x(xl))
    from_l = remote(pv.at[:, cols(xr)], near.at[slot(2)], at_x(xr))
    from_r = remote(pv.at[:, cols(xl)], near.at[slot(3)], at_x(xl))
    own = pltpu.make_async_copy(pv.at[:, cols(x)], near.at[slot(0)], local_sem.at[2])
    own.start()
    from_p = remote(pv.at[:, cols(x)], near.at[slot(1)], partner)
    i_p = remote(ids.at[:, slot(0)], ids.at[:, slot(1)], partner)
    i_l = remote(ids.at[:, slot(0)], ids.at[:, slot(2)], at_x(xr))
    i_r = remote(ids.at[:, slot(0)], ids.at[:, slot(3)], at_x(xl))
    i_o = remote(ids.at[:, slot(0)], ids.at[:, slot(6)], at_x(xo))
    c_p = remote(c_hbm, cv.at[1], partner)

    best[...] = jnp.full(best.shape, jnp.inf, jnp.float32)

    def distances(s):
        def tile(t, carry):
            part = cv[s, pl.ds(pl.multiple_of(t * TILE, TILE), TILE), :]
            inner = lax.dot_general(
                part, pv[...], (((1,), (1,)), ((), ())), preferred_element_type=jnp.float32
            )
            wide = part.astype(jnp.float32)
            square = jnp.sum(wide * wide, axis=1, keepdims=True)
            dist = square - 2.0 * inner
            low = jnp.min(dist.reshape(TILE // 8, 8, 512), axis=0)
            best[...] = jnp.minimum(best[...], low)
            return carry

        lax.fori_loop(0, 2048 // TILE, tile, 0)

    def accumulate(pair, yc, first=False):
        where = pl.ds(pair * 1024, 1024)
        base = m * 2048 + yc * CROWS

        def tile(t, carry):
            rows = pl.ds(pl.multiple_of(t * TILE, TILE), TILE)
            at = lax.broadcasted_iota(jnp.int32, (TILE, 1024), 0)
            hit = jnp.where(at == ids[:, where] - (base + t * TILE), 1.0, 0.0)
            part = jnp.dot(hit.astype(jnp.bfloat16), near[where, :], preferred_element_type=jnp.float32)
            count = sum(hit[:, k * LANES : (k + 1) * LANES] for k in range(1024 // LANES))
            if first:
                acc[yc, rows, :] = part
                cnt[yc, rows, :] = count
            else:
                acc[yc, rows, :] += part
                cnt[yc, rows, :] += count
            return carry

        lax.fori_loop(0, CROWS // TILE, tile, 0)

    def accumulate_all(pair, first=False):
        def body(yc, carry):
            accumulate(pair, yc, first)
            return carry

        lax.fori_loop(0, NY, body, 0)

    load_c.wait()
    distances(0)
    own.wait()
    from_p.wait_recv()
    i_p.wait_recv()
    accumulate_all(0, True)
    relay_l.wait_recv()
    on_l = remote(relay.at[0], near.at[pl.ds(6 * 512, 256)], at_x(xr))
    relay_r.wait_recv()
    on_r = remote(relay.at[1], near.at[pl.ds(6 * 512 + 256, 256)], at_x(xl))
    c_p.wait_recv()
    distances(1)
    from_l.wait_recv()
    i_l.wait_recv()
    p_l = remote(near.at[slot(2)], near.at[slot(4)], partner)
    pi_l = remote(ids.at[:, slot(2)], ids.at[:, slot(4)], partner)
    from_r.wait_recv()
    i_r.wait_recv()
    p_r = remote(near.at[slot(3)], near.at[slot(5)], partner)
    pi_r = remote(ids.at[:, slot(3)], ids.at[:, slot(5)], partner)
    accumulate_all(1)
    p_l.wait_recv()
    pi_l.wait_recv()
    p_r.wait_recv()
    pi_r.wait_recv()
    accumulate_all(2)
    on_l.wait_recv()
    on_r.wait_recv()
    i_o.wait_recv()
    p_o = remote(near.at[slot(6)], near.at[slot(7)], partner)
    pi_o = remote(ids.at[:, slot(6)], ids.at[:, slot(7)], partner)

    eye = lane_eye(LANES)
    for b in range(4):
        part = pv[pl.ds(b * LANES, LANES), :].astype(jnp.float32)
        square = to_row(jnp.sum(part * part, axis=1, keepdims=True), eye)
        lanes = pl.ds(b * LANES, LANES)
        cost_ref[:, lanes] = (square + jnp.min(best[:, lanes], axis=0, keepdims=True)) * (1.0 / 1024)

    p_o.wait_recv()
    pi_o.wait_recv()

    def pack(yc, rows_of, aux, words):
        def block(b, carry):
            eye = lane_eye(LANES)
            rows = pl.ds(pl.multiple_of(b * LANES, LANES), LANES)
            code, step = encode(acc[yc, rows, :])
            words(b, rows, code)
            aux[pl.ds(b, 1), :] = to_row(step, eye)
            if rows_of:
                count = jnp.sum(cnt[yc, rows, :], axis=1, keepdims=True)
                aux[pl.ds(4 + b, 1), :] = to_row(count, eye)
            return carry

        lax.fori_loop(0, CROWS // LANES, block, 0)

    def y_words(k):
        def put(b, rows, code):
            ysend[k, rows, :] = code

        return put

    accumulate(3, yo)
    pack(yo, True, yaux.at[2], y_words(2))
    yrelay_l = remote(ysend.at[2, lo], yrecv.at[3, lo], at_y(yr))
    yrelay_r = remote(ysend.at[2, hi], yrecv.at[3, hi], at_y(yl))
    ya_o = remote(yaux.at[2], yauxr.at[2], at_y(yo))
    accumulate(3, yr)
    pack(yr, True, yaux.at[0], y_words(0))
    y_l = remote(ysend.at[0], yrecv.at[0], at_y(yr))
    ya_l = remote(yaux.at[0], yauxr.at[0], at_y(yr))
    accumulate(3, yl)
    pack(yl, True, yaux.at[1], y_words(1))
    y_r = remote(ysend.at[1], yrecv.at[1], at_y(yl))
    ya_r = remote(yaux.at[1], yauxr.at[1], at_y(yl))
    accumulate(3, y)
    yrelay_l.wait_recv()
    yon_l = remote(yrecv.at[3, lo], yrecv.at[2, lo], at_y(yr))
    yrelay_r.wait_recv()
    yon_r = remote(yrecv.at[3, hi], yrecv.at[2, hi], at_y(yl))

    def unpack(k):
        def block(b, carry):
            eye = lane_eye(LANES)
            rows = pl.ds(pl.multiple_of(b * LANES, LANES), LANES)
            step = to_col(yauxr[k, pl.ds(b, 1), :], eye)
            high, low = decode(yrecv[k, rows, :], step)
            acc[y, rows, :LANES] += high
            acc[y, rows, LANES:] += low
            return carry

        lax.fori_loop(0, CROWS // LANES, block, 0)

    for k, copies in enumerate(((y_l, ya_l), (y_r, ya_r), (yon_l, yon_r, ya_o))):
        for copy in copies:
            copy.wait_recv()
        unpack(k)

    def z_words(b, rows, code):
        zsend[b] = code

    pack(y, True, zaux, z_words)
    zaux[pl.ds(4, 4), :] += yauxr[0, pl.ds(4, 4), :] + yauxr[1, pl.ds(4, 4), :] + yauxr[2, pl.ds(4, 4), :]
    zcopies = {}
    for d in (4, 3, 5, 2, 6, 1, 7):
        to = zat(d)
        piece = zsend.at[to // 2, pl.ds(pl.multiple_of(lax.rem(to, 2) * OWN, OWN), OWN)]
        zcopies[d] = (
            remote(piece, zrecv.at[d - 1], at_z(to)),
            remote(zaux, zauxr.at[d - 1], at_z(to)),
        )
    mine = lane_eye(OWN, lax.rem(z, 2) * OWN)
    zrow = z // 2
    sums = acc[y, pl.ds(pl.multiple_of(z * OWN, OWN), OWN), :]
    first, second = sums[:, :LANES], sums[:, LANES:]
    counts = zaux[pl.ds(4 + zrow, 1), :]
    for d in (1, 7, 2, 6, 3, 5, 4):
        for copy in zcopies[d]:
            copy.wait_recv()
        high, low = decode(zrecv[d - 1], to_col(zauxr[d - 1, pl.ds(zrow, 1), :], mine))
        first, second = first + high, second + low
        counts = counts + zauxr[d - 1, pl.ds(4 + zrow, 1), :]
    count = to_col(counts, mine)
    prior = cv[0, pl.ds(pl.multiple_of((y * NZ + z) * OWN, OWN), OWN), cols(x)].astype(jnp.float32)
    sums = jnp.concatenate([first, second], axis=1)
    fresh = jnp.where(count > 0.5, sums / jnp.maximum(count, 1.0), prior)
    code, step = encode(fresh)
    words_ref[x, y, z] = code
    steps_ref[x, y, z] = to_row(step, lane_eye(OWN))

    bh, ch = pl.ds(0, 32), pl.ds(32, 32)

    class HalfB:
        near_r, near_l, at, up = xr, xl, staticmethod(at_x), True

        @staticmethod
        def first(device):
            return [
                remote(words_ref.at[x, y, z, bh], words_ref.at[x, y, z, bh], device),
                remote(steps_ref.at[x, y, z], steps_ref.at[x, y, z], device),
            ]

        @staticmethod
        def group(along, zc, device):
            return [
                remote(words_ref.at[along, :, zc, bh], words_ref.at[along, :, zc, bh], device),
                remote(steps_ref.at[along, :, zc], steps_ref.at[along, :, zc], device),
            ]

    class HalfC:
        near_r, near_l, at, up = yr, yl, staticmethod(at_y), False

        @staticmethod
        def first(device):
            return [remote(words_ref.at[x, y, z, ch], words_ref.at[x, y, z, ch], device)]

        @staticmethod
        def group(along, zc, device):
            return [remote(words_ref.at[:, along, zc, ch], words_ref.at[:, along, zc, ch], device)]

    def arrive(copies):
        for copy in copies:
            copy.wait_recv()

    halves = (HalfB, HalfC)
    mine_at = {HalfB: x, HalfC: y}
    start = [HalfB.first(at_y(to)) for to in (yo, yr, yl)] + [HalfC.first(at_x(to)) for to in (xo, xr, xl)]
    for copies in start:
        arrive(copies)
    came = {h: {} for h in halves}
    side = {h: {} for h in halves}
    last = {h: {} for h in halves}

    def spread(h, d):
        along, zc = mine_at[h], zat(d)
        side[h][d] = (
            h.group(along, zc, h.at(h.near_r)),
            h.group(along, zc, h.at(h.near_l)),
        )

    def across(h, d):
        zc = zat(d)
        from_left, from_right = side[h][d]
        if d % 2 == 0:
            arrive(from_left)
            last[h][d] = (h.group(h.near_l, zc, h.at(h.near_r)), from_right)
        else:
            arrive(from_right)
            last[h][d] = (h.group(h.near_r, zc, h.at(h.near_l)), from_left)

    for h in halves:
        along = mine_at[h]
        came[h][-1] = h.group(along, z, at_z(zat(1)))
        came[h][1] = h.group(along, z, at_z(zat(-1)))
    for h in halves:
        along = mine_at[h]
        came[h][-2] = h.group(along, z, at_z(zat(2)))
        came[h][2] = h.group(along, z, at_z(zat(-2)))
    for h in halves:
        spread(h, 0)
    for h in halves:
        for d in (-1, 1):
            arrive(came[h][d])
            spread(h, d)
    for h in halves:
        along = mine_at[h]
        for d in (-2, 2):
            arrive(came[h][d])
            step_to = 1 if d < 0 else -1
            came[h][d - step_to] = h.group(along, zat(d), at_z(zat(step_to)))
            spread(h, d)
    for h in halves:
        across(h, 0)
    for h in halves:
        along = mine_at[h]
        for d in (-3, 3):
            arrive(came[h][d])
            if (d < 0) == h.up:
                step_to = 1 if d < 0 else -1
                came[h][4] = h.group(along, zat(d), at_z(zat(step_to)))
            spread(h, d)
    for h in halves:
        for d in (-1, 1):
            across(h, d)
    for h in halves:
        arrive(came[h][4])
        spread(h, 4)
    for h in halves:
        for d in (-2, 2, -3, 3, 4):
            across(h, d)
    for h in halves:
        for d in (0, -1, 1, -2, 2, -3, 3, 4):
            for copies in last[h][d]:
                arrive(copies)
    for copy in used:
        copy.wait_send()
    assert len(used) == N_COPIES, len(used)


N_COPIES = 143


def decode_kernel(words_ref, steps_ref, out_ref):
    eye = lane_eye(OWN)
    for xc in range(NX):
        for zc in range(NZ):
            step = to_col(steps_ref[xc, 0, zc], eye)
            high, low = decode(words_ref[xc, 0, zc], step)
            rows = pl.ds(zc * OWN, OWN)
            out_ref[rows, xc * FEATS : xc * FEATS + LANES] = high
            out_ref[rows, xc * FEATS + LANES : (xc + 1) * FEATS] = low


def shards(points, centroids, assign, keep_mask):
    vmem = pl.BlockSpec(memory_space=pltpu.VMEM)
    anywhere = pl.BlockSpec(memory_space=pl.ANY)
    dma = pltpu.SemaphoreType.DMA
    f32, i32, bf16 = jnp.float32, jnp.int32, jnp.bfloat16
    words, steps, cost = pl.pallas_call(
        update_kernel,
        out_shape=(
            jax.ShapeDtypeStruct((NX, NY, NZ, OWN, LANES), i32),
            jax.ShapeDtypeStruct((NX, NY, NZ, 1, LANES), f32),
            jax.ShapeDtypeStruct((1, 512), f32),
        ),
        in_specs=[anywhere, anywhere, vmem, vmem],
        out_specs=(vmem, vmem, vmem),
        scratch_shapes=[
            pltpu.VMEM((512, 1024), bf16),
            pltpu.VMEM((2, 2048, 1024), bf16),
            pltpu.VMEM((4096, FEATS), bf16),
            pltpu.VMEM((1, 4096), i32),
            pltpu.VMEM((2, 256, FEATS), bf16),
            pltpu.VMEM((8, 512), f32),
            pltpu.VMEM((NY, CROWS, FEATS), f32),
            pltpu.VMEM((NY, CROWS, LANES), f32),
            pltpu.VMEM((3, CROWS, LANES), i32),
            pltpu.VMEM((3, 8, LANES), f32),
            pltpu.VMEM((4, CROWS, LANES), i32),
            pltpu.VMEM((3, 8, LANES), f32),
            pltpu.VMEM((4, LANES, LANES), i32),
            pltpu.VMEM((8, LANES), f32),
            pltpu.VMEM((NZ - 1, OWN, LANES), i32),
            pltpu.VMEM((NZ - 1, 8, LANES), f32),
            dma((N_COPIES,)), dma((N_COPIES,)), dma((3,)),
        ],
        compiler_params=pltpu.CompilerParams(
            collective_id=0, has_side_effects=True, vmem_limit_bytes=48 * 1024 * 1024
        ),
    )(points, centroids, assign.reshape(1, 512), keep_mask.reshape(1, 512))
    new_centroids = pl.pallas_call(
        decode_kernel,
        grid=(NY,),
        out_shape=jax.ShapeDtypeStruct((2048, 1024), f32),
        in_specs=[
            pl.BlockSpec((NX, 1, NZ, OWN, LANES), lambda i: (0, i, 0, 0, 0)),
            pl.BlockSpec((NX, 1, NZ, 1, LANES), lambda i: (0, i, 0, 0, 0)),
        ],
        out_specs=pl.BlockSpec((CROWS, 1024), lambda i: (i, 0)),
        cost_estimate=pl.CostEstimate(flops=8 << 20, bytes_accessed=12 << 20, transcendentals=0),
    )(words, steps)
    return new_centroids, cost.reshape(512)


def solution(mesh):
    grid = Mesh(mesh.devices.reshape(NZ, NY, NX, 2), ("z", "y", "x", "mp"))
    rows = ("z", "y", "x", "mp")
    in_specs = (P(rows, None), P("mp", None), P(rows), P(rows))
    out_specs = (P("mp", None), P(rows))
    return jax.shard_map(shards, mesh=grid, in_specs=in_specs, out_specs=out_specs, check_vma=False)
```

```python
import jax
import jax.numpy as jnp
from jax import lax
from jax.experimental import pallas as pl
from jax.experimental.pallas import tpu as pltpu
from jax.sharding import Mesh
from jax.sharding import PartitionSpec as P

STEPS = 32000.0
TINY = 2.0**-100
N, NZ = 4, 8
LANES = 128
CROWS = 512
OWN = 64
PAIRS = OWN // 2
TILE = 256
ROWS = 512
MESH_ID = pl.DeviceIdType.MESH


def encode(v):
    top = jnp.maximum(jnp.max(jnp.abs(v), axis=1, keepdims=True), TINY)
    code = jnp.floor(v * (STEPS / top) + 0.5).astype(jnp.int32)
    return code, top * (1.0 / STEPS)


def pair(code):
    return (code[:PAIRS] << 16) | (code[PAIRS:] & 0xFFFF)


def decode(words, step):
    high = (words >> 16).astype(jnp.float32)
    low = ((words << 16) >> 16).astype(jnp.float32)
    return high * step[:PAIRS], low * step[PAIRS:]


def lane_eye(rows, shift=0):
    at_row = lax.broadcasted_iota(jnp.int32, (rows, LANES), 0)
    at_lane = lax.broadcasted_iota(jnp.int32, (rows, LANES), 1)
    return at_lane == at_row + shift


def to_row(col, eye):
    return jnp.sum(jnp.where(eye, col, 0.0), axis=0, keepdims=True)


def to_col(row, eye):
    return jnp.sum(jnp.where(eye, row, 0.0), axis=1, keepdims=True)


def update_kernel(
    p_hbm, c_hbm, assign_hbm, keep_hbm, words_ref, steps_ref, cost_ref,
    pv, cv, idv, near0, near, ids0, ids, relay, best, acc, cnt,
    ysend, yaux, yrecv, yauxr, zsend, zaux, zrecv, zauxr,
    send_sem, recv_sem, local_sem,
):
    z, y, x, m = (lax.axis_index(n) for n in ("z", "y", "x", "mp"))
    zat = lambda d: lax.rem(z + d + NZ, NZ)
    used = []
    scopes = []

    def phase(name):
        if scopes:
            scopes.pop().__exit__(None, None, None)
        if name:
            scopes.append(jax.named_scope(name))
            scopes[-1].__enter__()

    def remote(src, dst, device):
        k = len(used)
        copy = pltpu.make_async_remote_copy(
            src_ref=src, dst_ref=dst, send_sem=send_sem.at[k], recv_sem=recv_sem.at[k],
            device_id=device, device_id_type=MESH_ID,
        )
        copy.start()
        used.append(copy)
        return copy

    def arrive(copies):
        for copy in copies:
            copy.wait_recv()

    at_x = lambda to: (z, y, to, m)
    at_y = lambda to: (z, to, x, m)
    at_z = lambda to: (to, y, x, m)
    partner = (z, y, x, 1 - m)

    class Colour:
        def __init__(self, c, first, second, at_first, at_second):
            self.c, self.f, self.r = c, first, second
            self.fr, self.fl, self.fo = (lax.rem(first + d, N) for d in (1, 3, 2))
            self.rr, self.rl, self.ro = (lax.rem(second + d, N) for d in (1, 3, 2))
            self.at_f, self.at_r = at_first, at_second

        def cols(self, f):
            return pl.ds(pl.multiple_of(self.c * 512 + f * LANES, LANES), LANES)

    colours = (Colour(0, x, y, at_x, at_y), Colour(1, y, x, at_y, at_x))

    phase("enter")
    loads = [
        pltpu.make_async_copy(p_hbm, pv, local_sem.at[0]),
        pltpu.make_async_copy(assign_hbm, idv.at[0], local_sem.at[1]),
        pltpu.make_async_copy(keep_hbm, idv.at[1], local_sem.at[2]),
    ]
    load_c = pltpu.make_async_copy(c_hbm, cv.at[0], local_sem.at[3])
    for copy in loads + [load_c]:
        copy.start()

    peers = [partner] + [at_z(zat(d)) for d in range(1, NZ)]
    for k in colours:
        peers += [k.at_f(k.fr), k.at_f(k.fl), k.at_f(k.fo)]
    barrier = pltpu.get_barrier_semaphore()
    for peer in peers:
        pl.semaphore_signal(barrier, inc=1, device_id=peer, device_id_type=MESH_ID)
    for copy in loads:
        copy.wait()
    ids0[:, :ROWS] = jnp.where(idv[1] > 0, idv[0], -1)
    best[...] = jnp.full(best.shape, jnp.inf, jnp.float32)
    pl.semaphore_wait(barrier, len(peers))

    phase("send_p")

    def slot(s):
        return pl.ds((s - 2) * ROWS, ROWS)

    lo, hi = pl.ds(0, ROWS // 2), pl.ds(ROWS // 2, ROWS // 2)
    mine_ids = ids0.at[:, pl.ds(0, ROWS)]
    for k in colours:
        k.relay_l = remote(pv.at[lo, k.cols(k.fo)], relay.at[k.c, 0], k.at_f(k.fr))
        k.relay_r = remote(pv.at[hi, k.cols(k.fo)], relay.at[k.c, 1], k.at_f(k.fl))
    own = []
    from_p = [remote(mine_ids, ids0.at[:, pl.ds(ROWS, ROWS)], partner)]
    for k in colours:
        lanes = pl.ds(k.c * LANES, LANES)
        own.append(
            pltpu.make_async_copy(pv.at[:, k.cols(k.f)], near0.at[pl.ds(0, ROWS), lanes], local_sem.at[4 + k.c])
        )
        own[-1].start()
        from_p.append(remote(pv.at[:, k.cols(k.f)], near0.at[pl.ds(ROWS, ROWS), lanes], partner))
    for k in colours:
        k.from_l = [
            remote(mine_ids, ids.at[k.c, :, slot(2)], k.at_f(k.fr)),
            remote(pv.at[:, k.cols(k.fr)], near.at[k.c, slot(2)], k.at_f(k.fr)),
        ]
        k.from_r = [
            remote(mine_ids, ids.at[k.c, :, slot(3)], k.at_f(k.fl)),
            remote(pv.at[:, k.cols(k.fl)], near.at[k.c, slot(3)], k.at_f(k.fl)),
        ]
        k.from_o = [remote(mine_ids, ids.at[k.c, :, slot(6)], k.at_f(k.fo))]
    c_p = remote(c_hbm, cv.at[1], partner)

    def distances(s, first, count):
        def tile(t, carry):
            part = cv[s, pl.ds(pl.multiple_of(t * TILE, TILE), TILE), :]
            inner = lax.dot_general(
                part, pv[...], (((1,), (1,)), ((), ())), preferred_element_type=jnp.float32
            )
            wide = part.astype(jnp.float32)
            square = jnp.sum(wide * wide, axis=1, keepdims=True)
            dist = square - 2.0 * inner
            low = jnp.min(dist.reshape(TILE // 8, 8, ROWS), axis=0)
            best[...] = jnp.minimum(best[...], low)
            return carry

        lax.fori_loop(first, first + count, tile, 0)

    def hits(id_row, base):
        local = id_row - base
        local = jnp.where((local >= 0) & (local < TILE), local, -1).astype(jnp.float32)
        local = jnp.broadcast_to(local, (16, 2 * ROWS)).astype(jnp.bfloat16)
        at = lax.broadcasted_iota(jnp.int32, (TILE, LANES), 0).astype(jnp.float32).astype(jnp.bfloat16)
        at = at.reshape(TILE // 16, 16, LANES)
        one, zero = jnp.ones((), jnp.bfloat16), jnp.zeros((), jnp.bfloat16)
        parts = [
            jnp.where(at == local[None, :, i * LANES : (i + 1) * LANES], one, zero).reshape(TILE, LANES)
            for i in range(2 * ROWS // LANES)
        ]
        count = parts[0]
        for part in parts[1:]:
            count = count + part
        return jnp.concatenate(parts, axis=1), count

    def accumulate(k, two, q):
        where = pl.ds((two - 1) * 2 * ROWS, 2 * ROWS)

        def tile(t, carry):
            rows = pl.ds(pl.multiple_of(t * TILE, TILE), TILE)
            hit, count = hits(ids[k.c, :, where], m * 2048 + q * CROWS + t * TILE)
            acc[k.c, q, rows, :] += jnp.dot(hit, near[k.c, where, :], preferred_element_type=jnp.float32)
            cnt[k.c, q, rows, :] += count
            return carry

        lax.fori_loop(0, CROWS // TILE, tile, 0)

    def accumulate_all(k, two):
        def body(q, carry):
            accumulate(k, two, q)
            return carry

        lax.fori_loop(0, N, body, 0)

    def accumulate_own():
        def tile(t, carry):
            q, rows = t // 2, pl.ds(pl.multiple_of(lax.rem(t, 2) * TILE, TILE), TILE)
            hit, count = hits(ids0[...], m * 2048 + t * TILE)
            part = jnp.dot(hit, near0[...], preferred_element_type=jnp.float32)
            for c in range(2):
                acc[c, q, rows, :] = part[:, c * LANES : (c + 1) * LANES]
                cnt[c, q, rows, :] = count
            return carry

        lax.fori_loop(0, 2048 // TILE, tile, 0)

    phase("dist0a")
    load_c.wait()
    distances(0, 0, 4)
    phase("w_own")
    for copy in own:
        copy.wait()
    arrive(from_p)
    phase("acc0")
    accumulate_own()
    phase("w_relay")
    for k in colours:
        k.relay_l.wait_recv()
        k.from_o.append(remote(relay.at[k.c, 0], near.at[k.c, pl.ds(4 * ROWS, ROWS // 2)], k.at_f(k.fr)))
        k.relay_r.wait_recv()
        k.from_o.append(remote(relay.at[k.c, 1], near.at[k.c, pl.ds(4 * ROWS + ROWS // 2, ROWS // 2)], k.at_f(k.fl)))
    phase("dist0b")
    distances(0, 4, 4)

    def to_partner(k, source, target):
        return [
            remote(near.at[k.c, slot(source)], near.at[k.c, slot(target)], partner),
            remote(ids.at[k.c, :, slot(source)], ids.at[k.c, :, slot(target)], partner),
        ]

    phase("w_lr")
    for k in colours:
        arrive(k.from_l)
        k.two = to_partner(k, 2, 4)
        arrive(k.from_r)
        k.two += to_partner(k, 3, 5)
    phase("acc1")
    accumulate_all(colours[0], 1)
    phase("w_o")
    for k in colours:
        arrive(k.from_o)
        k.three = to_partner(k, 6, 7)
    phase("acc1b")
    accumulate_all(colours[1], 1)
    phase("w_plr")
    for k in colours:
        arrive(k.two)
    phase("acc2")
    for k in colours:
        accumulate_all(k, 2)
    phase("w_po")
    for k in colours:
        arrive(k.three)

    def pack(c, q, words, aux):
        def block(b, carry):
            eye = lane_eye(LANES)
            rows = pl.ds(pl.multiple_of(b * LANES, LANES), LANES)
            code, step = encode(acc[c, q, rows, :])
            for j in range(2):
                words(2 * b + j)[...] = pair(code[j * OWN : (j + 1) * OWN])
            count = jnp.sum(cnt[c, q, rows, :].astype(jnp.float32), axis=1, keepdims=True)
            aux(b, to_row(step, eye), to_row(count, eye))
            return carry

        lax.fori_loop(0, CROWS // LANES, block, 0)

    def pack_y(k, q, s):
        def aux(b, step, count):
            yaux[k.c, s, b, 0:1, :] = step
            yaux[k.c, s, b, 1:2, :] = count

        accumulate(k, 3, q)
        pack(k.c, q, lambda zb: ysend.at[k.c, s, zb], aux)

    h0, h1 = pl.ds(0, NZ // 2), pl.ds(NZ // 2, NZ // 2)
    phase("y_pack")
    for k in colours:
        pack_y(k, k.ro, 2)
        k.yrelay_l = remote(ysend.at[k.c, 2, h0], yrecv.at[k.c, 3, h0], k.at_r(k.rr))
        k.yrelay_r = remote(ysend.at[k.c, 2, h1], yrecv.at[k.c, 3, h1], k.at_r(k.rl))
        k.y_o = [remote(yaux.at[k.c, 2], yauxr.at[k.c, 2], k.at_r(k.ro))]
    for k in colours:
        pack_y(k, k.rr, 0)
        k.y_l = [
            remote(yaux.at[k.c, 0], yauxr.at[k.c, 0], k.at_r(k.rr)),
            remote(ysend.at[k.c, 0], yrecv.at[k.c, 0], k.at_r(k.rr)),
        ]
        pack_y(k, k.rl, 1)
        k.y_r = [
            remote(yaux.at[k.c, 1], yauxr.at[k.c, 1], k.at_r(k.rl)),
            remote(ysend.at[k.c, 1], yrecv.at[k.c, 1], k.at_r(k.rl)),
        ]
    phase("y_relay")
    for k in colours:
        k.yrelay_l.wait_recv()
        k.y_o.append(remote(yrecv.at[k.c, 3, h0], yrecv.at[k.c, 2, h0], k.at_r(k.rr)))
        k.yrelay_r.wait_recv()
        k.y_o.append(remote(yrecv.at[k.c, 3, h1], yrecv.at[k.c, 2, h1], k.at_r(k.rl)))
    for k in colours:
        accumulate(k, 3, k.r)

    def unpack(k, s):
        def block(b, carry):
            step = to_col(yauxr[k.c, s, b, 0:1, :], lane_eye(LANES))
            for j in range(2):
                high, low = decode(yrecv[k.c, s, 2 * b + j], step[j * OWN : (j + 1) * OWN])
                base = pl.multiple_of(b * LANES, LANES) + j * OWN
                acc[k.c, k.r, pl.ds(base, PAIRS), :] += high
                acc[k.c, k.r, pl.ds(base + PAIRS, PAIRS), :] += low
            return carry

        lax.fori_loop(0, CROWS // LANES, block, 0)

    phase("y_unpack")
    for k in colours:
        arrive(k.y_l)
        unpack(k, 0)
        arrive(k.y_r)
        unpack(k, 1)
    phase("y_unpack_o")
    for k in colours:
        arrive(k.y_o)
        unpack(k, 2)

    phase("z_pack")
    for k in colours:
        def aux(b, step, count, k=k):
            zaux[b, 2 * k.c : 2 * k.c + 1, :] = step
            for s in range(3):
                count = count + yauxr[k.c, s, b, 1:2, :]
            zaux[b, 2 * k.c + 1 : 2 * k.c + 2, :] = count

        pack(k.c, k.r, lambda zb, k=k: zsend.at[zb, k.c], aux)
    zcopies = {}
    for d in (4, 3, 5, 2, 6, 1, 7):
        to = zat(d)
        zcopies[d] = [
            remote(zaux.at[to // 2], zauxr.at[d - 1], at_z(to)),
            remote(zsend.at[to], zrecv.at[d - 1], at_z(to)),
        ]
    phase("dist1")
    c_p.wait_recv()
    distances(1, 0, 2048 // TILE)
    eye = lane_eye(LANES)
    for b in range(ROWS // LANES):
        part = pv[pl.ds(b * LANES, LANES), :].astype(jnp.float32)
        square = to_row(jnp.sum(part * part, axis=1, keepdims=True), eye)
        lanes = pl.ds(b * LANES, LANES)
        cost_ref[:, lanes] = (square + jnp.min(best[:, lanes], axis=0, keepdims=True)) * (1.0 / 1024)
    phase("z_sum")
    mine = lane_eye(OWN, lax.rem(z, 2) * OWN)
    for k in colours:
        sums = acc[k.c, k.r, pl.ds(pl.multiple_of(z * OWN, OWN), OWN), :]
        k.high, k.low = sums[:PAIRS], sums[PAIRS:]
        k.count = zaux[z // 2, 2 * k.c + 1 : 2 * k.c + 2, :]
    for d in (1, 7, 2, 6, 3, 5, 4):
        arrive(zcopies[d])
        for k in colours:
            step = to_col(zauxr[d - 1, 2 * k.c : 2 * k.c + 1, :], mine)
            high, low = decode(zrecv[d - 1, k.c], step)
            k.high, k.low = k.high + high, k.low + low
            k.count = k.count + zauxr[d - 1, 2 * k.c + 1 : 2 * k.c + 2, :]
    phase("fresh")
    for k in colours:
        count = to_col(k.count, mine)
        rows = pl.ds(pl.multiple_of((k.r * NZ + z) * OWN, OWN), OWN)
        prior = cv[0, rows, k.cols(k.f)].astype(jnp.float32)
        sums = jnp.concatenate([k.high, k.low], axis=0)
        code, step = encode(jnp.where(count > 0.5, sums / jnp.maximum(count, 1.0), prior))
        words_ref[k.c, k.f, k.r, z] = pair(code)
        steps_ref[k.c, k.f, k.r, z] = to_row(step, lane_eye(OWN))
        k.start = []
        for to in (k.ro, k.rr, k.rl):
            for ref in (steps_ref, words_ref):
                own_piece = ref.at[k.c, k.f, k.r, z]
                k.start.append(remote(own_piece, own_piece, k.at_r(to)))

    def group(k, f, zc, device):
        copies = []
        for ref in (steps_ref, words_ref):
            piece = ref.at[k.c, f, :, zc]
            copies.append(remote(piece, piece, device))
        return copies

    def hop(k, way, h, half):
        zc, device = zat(-way * (h - 1)), at_z(zat(way))
        copies = []
        if half == 0:
            piece = steps_ref.at[k.c, k.f, :, zc]
            copies.append(remote(piece, piece, device))
        piece = words_ref.at[k.c, k.f, pl.ds(half * (N // 2), N // 2), zc]
        copies.append(remote(piece, piece, device))
        k.hops[way, h, half] = copies

    def spread(k, d):
        zc = zat(d)
        k.side[d] = (group(k, k.f, zc, k.at_f(k.fr)), group(k, k.f, zc, k.at_f(k.fl)))

    def across(k, d):
        zc = zat(d)
        from_left, from_right = k.side[d]
        if d in (0, 1, 2, 3):
            arrive(from_left)
            k.last += group(k, k.fl, zc, k.at_f(k.fr)) + from_right
        else:
            arrive(from_right)
            k.last += group(k, k.fr, zc, k.at_f(k.fl)) + from_left

    phase("g1")
    for k in colours:
        arrive(k.start)
        k.hops, k.side, k.last = {}, {}, []
        for half in (0, 1):
            for way in (1, -1):
                hop(k, way, 1, half)
        spread(k, 0)
    for h in (1, 2, 3):
        phase(f"g_z{h}")
        for k in colours:
            for half in (0, 1):
                for way in (1, -1):
                    arrive(k.hops[way, h, half])
                    if h < 3 or way == (1, -1)[half]:
                        hop(k, way, h + 1, half)
            for way in (1, -1):
                spread(k, -way * h)
        phase(f"g_x{h}")
        for k in colours:
            for d in (0,) if h == 1 else (1 - h, h - 1):
                across(k, d)
    phase("g_z4")
    for k in colours:
        arrive(k.hops[1, 4, 0])
        arrive(k.hops[-1, 4, 1])
        spread(k, 4)
    phase("g_x4")
    for k in colours:
        for d in (-3, 3, 4):
            across(k, d)
    phase("g_last")
    for k in colours:
        arrive(k.last)
    phase("w_send")
    for copy in used:
        copy.wait_send()
    phase(None)
    assert len(used) == N_COPIES, len(used)


N_COPIES = 216


def decode_kernel(words_ref, steps_ref, cost_ref, out_hbm, cost_hbm, rows_ref, sems):
    put_cost = pltpu.make_async_copy(cost_ref, cost_hbm, sems.at[N])
    put_cost.start()
    puts = []
    for r in range(N):

        def block(zb, carry):
            eye = lane_eye(OWN)
            base = pl.multiple_of(zb * OWN, OWN)
            for c in range(2):
                for f in range(N):
                    step = to_col(steps_ref[c, f, r, zb], eye)
                    high, low = decode(words_ref[c, f, r, zb], step)
                    lanes = pl.ds((c * N + f) * LANES, LANES)
                    rows_ref[r, pl.ds(base, PAIRS), lanes] = high
                    rows_ref[r, pl.ds(base + PAIRS, PAIRS), lanes] = low
            return carry

        lax.fori_loop(0, NZ, block, 0)
        put = pltpu.make_async_copy(rows_ref.at[r], out_hbm.at[pl.ds(r * CROWS, CROWS)], sems.at[r])
        put.start()
        puts.append(put)
    for put in puts + [put_cost]:
        put.wait()


def shards(points, centroids, assign, keep_mask):
    vmem = pl.BlockSpec(memory_space=pltpu.VMEM)
    hbm = pl.BlockSpec(memory_space=pltpu.HBM)
    dma = pltpu.SemaphoreType.DMA
    f32, i32, bf16 = jnp.float32, jnp.int32, jnp.bfloat16
    args = (points, centroids, assign.reshape(1, ROWS), keep_mask.reshape(1, ROWS))
    words, steps, cost = pl.pallas_call(
        update_kernel,
        out_shape=(
            jax.ShapeDtypeStruct((2, N, N, NZ, PAIRS, LANES), i32),
            jax.ShapeDtypeStruct((2, N, N, NZ, 1, LANES), f32),
            jax.ShapeDtypeStruct((1, ROWS), f32),
        ),
        in_specs=[hbm] * 4,
        out_specs=(vmem, vmem, vmem),
        scratch_shapes=[
            pltpu.VMEM((ROWS, 1024), bf16),
            pltpu.VMEM((2, 2048, 1024), bf16),
            pltpu.VMEM((2, 1, ROWS), i32),
            pltpu.VMEM((2 * ROWS, 2 * LANES), bf16),
            pltpu.VMEM((2, 6 * ROWS, LANES), bf16),
            pltpu.VMEM((1, 2 * ROWS), i32),
            pltpu.VMEM((2, 1, 6 * ROWS), i32),
            pltpu.VMEM((2, 2, ROWS // 2, LANES), bf16),
            pltpu.VMEM((8, ROWS), f32),
            pltpu.VMEM((2, N, CROWS, LANES), f32),
            pltpu.VMEM((2, N, CROWS, LANES), bf16),
            pltpu.VMEM((2, 3, NZ, PAIRS, LANES), i32),
            pltpu.VMEM((2, 3, N, 2, LANES), f32),
            pltpu.VMEM((2, 4, NZ, PAIRS, LANES), i32),
            pltpu.VMEM((2, 3, N, 2, LANES), f32),
            pltpu.VMEM((NZ, 2, PAIRS, LANES), i32),
            pltpu.VMEM((N, 4, LANES), f32),
            pltpu.VMEM((NZ - 1, 2, PAIRS, LANES), i32),
            pltpu.VMEM((NZ - 1, 4, LANES), f32),
            dma((N_COPIES,)), dma((N_COPIES,)), dma((6,)),
        ],
        compiler_params=pltpu.CompilerParams(
            collective_id=0, has_side_effects=True, vmem_limit_bytes=40 * 1024 * 1024
        ),
    )(*(pltpu.with_memory_space_constraint(a, pltpu.HBM) for a in args))
    new_centroids, cost = pl.pallas_call(
        decode_kernel,
        out_shape=(jax.ShapeDtypeStruct((2048, 1024), f32), jax.ShapeDtypeStruct((1, ROWS), f32)),
        in_specs=[vmem] * 3,
        out_specs=(hbm, hbm),
        scratch_shapes=[pltpu.VMEM((N, CROWS, 1024), f32), dma((N + 1,))],
        compiler_params=pltpu.CompilerParams(vmem_limit_bytes=12 * 1024 * 1024),
        cost_estimate=pl.CostEstimate(flops=8 << 20, bytes_accessed=12 << 20, transcendentals=0),
    )(words, steps, cost)
    return new_centroids, cost.reshape(ROWS)


def solution(mesh):
    grid = Mesh(mesh.devices.reshape(NZ, N, N, 2), ("z", "y", "x", "mp"))
    rows = ("z", "y", "x", "mp")
    in_specs = (P(rows, None), P("mp", None), P(rows), P(rows))
    out_specs = (P("mp", None), P(rows))
    return jax.shard_map(shards, mesh=grid, in_specs=in_specs, out_specs=out_specs, check_vma=False)
```

```python
import jax
import jax.numpy as jnp
from jax import lax
from jax.experimental import pallas as pl
from jax.experimental.pallas import tpu as pltpu
from jax.sharding import Mesh
from jax.sharding import PartitionSpec as P

STEPS = 32000.0
TINY = 2.0**-100
N, NZ = 4, 8
LANES = 128
CROWS = 512
OWN = 64
PAIRS = OWN // 2
TILE = 256
ROWS = 512
MESH_ID = pl.DeviceIdType.MESH


def encode(v):
    top = jnp.maximum(jnp.max(jnp.abs(v), axis=1, keepdims=True), TINY)
    code = jnp.floor(v * (STEPS / top) + 0.5).astype(jnp.int32)
    return code, top * (1.0 / STEPS)


def pair(code):
    return (code[:PAIRS] << 16) | (code[PAIRS:] & 0xFFFF)


def decode(words, step):
    high = (words >> 16).astype(jnp.float32)
    low = ((words << 16) >> 16).astype(jnp.float32)
    return high * step[:PAIRS], low * step[PAIRS:]


def lane_eye(rows, shift=0):
    at_row = lax.broadcasted_iota(jnp.int32, (rows, LANES), 0)
    at_lane = lax.broadcasted_iota(jnp.int32, (rows, LANES), 1)
    return at_lane == at_row + shift


def to_row(col, eye):
    return jnp.sum(jnp.where(eye, col, 0.0), axis=0, keepdims=True)


def to_col(row, eye):
    return jnp.sum(jnp.where(eye, row, 0.0), axis=1, keepdims=True)


def update_kernel(
    p_hbm, c_hbm, assign_hbm, keep_hbm, out_ref, cost_ref,
    words_ref, steps_ref,
    pv, cv, idv, near0, near, ids0, ids, relay, best, acc, cnt,
    ysend, yaux, yrecv, yauxr, zsend, zaux, zrecv, zauxr,
    send_sem, recv_sem, local_sem,
):
    z, y, x, m = (lax.axis_index(n) for n in ("z", "y", "x", "mp"))
    zat = lambda d: lax.rem(z + d + NZ, NZ)
    used = []
    scopes = []

    def phase(name):
        if scopes:
            scopes.pop().__exit__(None, None, None)
        if name:
            scopes.append(jax.named_scope(name))
            scopes[-1].__enter__()

    def remote(src, dst, device):
        k = len(used)
        copy = pltpu.make_async_remote_copy(
            src_ref=src, dst_ref=dst, send_sem=send_sem.at[k], recv_sem=recv_sem.at[k],
            device_id=device, device_id_type=MESH_ID,
        )
        copy.start()
        used.append(copy)
        return copy

    def arrive(copies):
        for copy in copies:
            copy.wait_recv()

    at_x = lambda to: (z, y, to, m)
    at_y = lambda to: (z, to, x, m)
    at_z = lambda to: (to, y, x, m)
    partner = (z, y, x, 1 - m)

    class Colour:
        def __init__(self, c, first, second, at_first, at_second):
            self.c, self.f, self.r = c, first, second
            self.fr, self.fl, self.fo = (lax.rem(first + d, N) for d in (1, 3, 2))
            self.rr, self.rl, self.ro = (lax.rem(second + d, N) for d in (1, 3, 2))
            self.at_f, self.at_r = at_first, at_second

        def cols(self, f):
            return pl.ds(pl.multiple_of(self.c * 512 + f * LANES, LANES), LANES)

    colours = (Colour(0, x, y, at_x, at_y), Colour(1, y, x, at_y, at_x))

    phase("enter")
    loads = [
        pltpu.make_async_copy(p_hbm, pv, local_sem.at[0]),
        pltpu.make_async_copy(assign_hbm, idv.at[0], local_sem.at[1]),
        pltpu.make_async_copy(keep_hbm, idv.at[1], local_sem.at[2]),
    ]
    load_c = pltpu.make_async_copy(c_hbm, cv.at[0], local_sem.at[3])
    for copy in loads + [load_c]:
        copy.start()

    peers = [partner] + [at_z(zat(d)) for d in range(1, NZ)]
    for k in colours:
        peers += [k.at_f(k.fr), k.at_f(k.fl), k.at_f(k.fo)]
    barrier = pltpu.get_barrier_semaphore()
    for peer in peers:
        pl.semaphore_signal(barrier, inc=1, device_id=peer, device_id_type=MESH_ID)
    for copy in loads:
        copy.wait()
    ids0[:, :ROWS] = jnp.where(idv[1] > 0, idv[0], -1)
    best[...] = jnp.full(best.shape, jnp.inf, jnp.float32)
    pl.semaphore_wait(barrier, len(peers))

    phase("send_p")

    def slot(s):
        return pl.ds((s - 2) * ROWS, ROWS)

    lo, hi = pl.ds(0, ROWS // 2), pl.ds(ROWS // 2, ROWS // 2)
    mine_ids = ids0.at[:, pl.ds(0, ROWS)]
    for k in colours:
        k.relay_l = remote(pv.at[lo, k.cols(k.fo)], relay.at[k.c, 0], k.at_f(k.fr))
        k.relay_r = remote(pv.at[hi, k.cols(k.fo)], relay.at[k.c, 1], k.at_f(k.fl))
    own = []
    from_p = [remote(mine_ids, ids0.at[:, pl.ds(ROWS, ROWS)], partner)]
    for k in colours:
        lanes = pl.ds(k.c * LANES, LANES)
        own.append(
            pltpu.make_async_copy(pv.at[:, k.cols(k.f)], near0.at[pl.ds(0, ROWS), lanes], local_sem.at[4 + k.c])
        )
        own[-1].start()
        from_p.append(remote(pv.at[:, k.cols(k.f)], near0.at[pl.ds(ROWS, ROWS), lanes], partner))
    for k in colours:
        k.from_l = [
            remote(mine_ids, ids.at[k.c, :, slot(2)], k.at_f(k.fr)),
            remote(pv.at[:, k.cols(k.fr)], near.at[k.c, slot(2)], k.at_f(k.fr)),
        ]
        k.from_r = [
            remote(mine_ids, ids.at[k.c, :, slot(3)], k.at_f(k.fl)),
            remote(pv.at[:, k.cols(k.fl)], near.at[k.c, slot(3)], k.at_f(k.fl)),
        ]
        k.from_o = [remote(mine_ids, ids.at[k.c, :, slot(6)], k.at_f(k.fo))]
    c_p = remote(c_hbm, cv.at[1], partner)

    def distances(s, first, count):
        def tile(t, carry):
            part = cv[s, pl.ds(pl.multiple_of(t * TILE, TILE), TILE), :]
            inner = lax.dot_general(
                part, pv[...], (((1,), (1,)), ((), ())), preferred_element_type=jnp.float32
            )
            wide = part.astype(jnp.float32)
            square = jnp.sum(wide * wide, axis=1, keepdims=True)
            dist = square - 2.0 * inner
            low = jnp.min(dist.reshape(TILE // 8, 8, ROWS), axis=0)
            best[...] = jnp.minimum(best[...], low)
            return carry

        lax.fori_loop(first, first + count, tile, 0)

    def hits(id_row, base):
        local = id_row - base
        local = jnp.where((local >= 0) & (local < TILE), local, -1).astype(jnp.float32)
        local = jnp.broadcast_to(local, (16, 2 * ROWS)).astype(jnp.bfloat16)
        at = lax.broadcasted_iota(jnp.int32, (TILE, LANES), 0).astype(jnp.float32).astype(jnp.bfloat16)
        at = at.reshape(TILE // 16, 16, LANES)
        one, zero = jnp.ones((), jnp.bfloat16), jnp.zeros((), jnp.bfloat16)
        parts = [
            jnp.where(at == local[None, :, i * LANES : (i + 1) * LANES], one, zero).reshape(TILE, LANES)
            for i in range(2 * ROWS // LANES)
        ]
        count = parts[0]
        for part in parts[1:]:
            count = count + part
        return jnp.concatenate(parts, axis=1), count

    def hits_chunk(id_row, base):
        low, count_low = hits(id_row, base)
        high, count_high = hits(id_row, base + TILE)
        return jnp.concatenate([low, high], axis=0), jnp.concatenate([count_low, count_high], axis=0)

    def accumulate(c, two, q):
        where = pl.ds((two - 1) * 2 * ROWS, 2 * ROWS)
        hit, count = hits_chunk(ids[c, :, where], m * 2048 + q * CROWS)
        acc[c, q] += jnp.dot(hit, near[c, where, :], preferred_element_type=jnp.float32)
        cnt[c, q] += count

    def accumulate_all(c, two):
        def body(q, carry):
            accumulate(c, two, q)
            return carry

        lax.fori_loop(0, N, body, 0)

    def accumulate_own():
        def body(q, carry):
            hit, count = hits_chunk(ids0[...], m * 2048 + q * CROWS)
            part = jnp.dot(hit, near0[...], preferred_element_type=jnp.float32)
            for c in range(2):
                acc[c, q] = part[:, c * LANES : (c + 1) * LANES]
                cnt[c, q] = count
            return carry

        lax.fori_loop(0, N, body, 0)

    phase("dist0a")
    load_c.wait()
    distances(0, 0, 4)
    phase("w_own")
    for copy in own:
        copy.wait()
    arrive(from_p)
    phase("acc0")
    accumulate_own()
    phase("w_relay")
    for k in colours:
        k.relay_l.wait_recv()
        k.from_o.append(remote(relay.at[k.c, 0], near.at[k.c, pl.ds(4 * ROWS, ROWS // 2)], k.at_f(k.fr)))
        k.relay_r.wait_recv()
        k.from_o.append(remote(relay.at[k.c, 1], near.at[k.c, pl.ds(4 * ROWS + ROWS // 2, ROWS // 2)], k.at_f(k.fl)))
    phase("dist0b")
    distances(0, 4, 4)

    def to_partner(k, source, target):
        return [
            remote(near.at[k.c, slot(source)], near.at[k.c, slot(target)], partner),
            remote(ids.at[k.c, :, slot(source)], ids.at[k.c, :, slot(target)], partner),
        ]

    phase("w_lr")
    for k in colours:
        arrive(k.from_l)
        k.two = to_partner(k, 2, 4)
        arrive(k.from_r)
        k.two += to_partner(k, 3, 5)
    phase("acc1")
    accumulate_all(0, 1)
    phase("w_o")
    for k in colours:
        arrive(k.from_o)
        k.three = to_partner(k, 6, 7)
    phase("acc1b")
    accumulate_all(1, 1)
    phase("w_plr")
    for k in colours:
        arrive(k.two)
    phase("acc2")
    for k in colours:
        accumulate_all(k.c, 2)
    phase("w_po")
    for k in colours:
        arrive(k.three)

    def pack(c, q, words, aux):
        def block(b, carry):
            eye = lane_eye(LANES)
            rows = pl.ds(pl.multiple_of(b * LANES, LANES), LANES)
            code, step = encode(acc[c, q, rows, :])
            for j in range(2):
                words(2 * b + j)[...] = pair(code[j * OWN : (j + 1) * OWN])
            count = jnp.sum(cnt[c, q, rows, :].astype(jnp.float32), axis=1, keepdims=True)
            aux(b, to_row(step, eye), to_row(count, eye))
            return carry

        lax.fori_loop(0, CROWS // LANES, block, 0, unroll=True)

    def pack_y(k, q, s):
        def aux(b, step, count):
            yaux[k.c, s, b, 0:1, :] = step
            yaux[k.c, s, b, 1:2, :] = count

        accumulate(k.c, 3, q)
        pack(k.c, q, lambda zb: ysend.at[k.c, s, zb], aux)

    h0, h1 = pl.ds(0, NZ // 2), pl.ds(NZ // 2, NZ // 2)
    phase("y_pack")
    for k in colours:
        pack_y(k, k.ro, 2)
        k.yrelay_l = remote(ysend.at[k.c, 2, h0], yrecv.at[k.c, 3, h0], k.at_r(k.rr))
        k.yrelay_r = remote(ysend.at[k.c, 2, h1], yrecv.at[k.c, 3, h1], k.at_r(k.rl))
        k.y_o = [remote(yaux.at[k.c, 2], yauxr.at[k.c, 2], k.at_r(k.ro))]
    for k in colours:
        pack_y(k, k.rr, 0)
        k.y_l = [
            remote(yaux.at[k.c, 0], yauxr.at[k.c, 0], k.at_r(k.rr)),
            remote(ysend.at[k.c, 0], yrecv.at[k.c, 0], k.at_r(k.rr)),
        ]
        pack_y(k, k.rl, 1)
        k.y_r = [
            remote(yaux.at[k.c, 1], yauxr.at[k.c, 1], k.at_r(k.rl)),
            remote(ysend.at[k.c, 1], yrecv.at[k.c, 1], k.at_r(k.rl)),
        ]
    phase("y_relay")
    for k in colours:
        k.yrelay_l.wait_recv()
        k.y_o.append(remote(yrecv.at[k.c, 3, h0], yrecv.at[k.c, 2, h0], k.at_r(k.rr)))
        k.yrelay_r.wait_recv()
        k.y_o.append(remote(yrecv.at[k.c, 3, h1], yrecv.at[k.c, 2, h1], k.at_r(k.rl)))
    for k in colours:
        accumulate(k.c, 3, k.r)

    def unpack(k, s):
        def block(b, carry):
            step = to_col(yauxr[k.c, s, b, 0:1, :], lane_eye(LANES))
            for j in range(2):
                high, low = decode(yrecv[k.c, s, 2 * b + j], step[j * OWN : (j + 1) * OWN])
                base = pl.multiple_of(b * LANES, LANES) + j * OWN
                acc[k.c, k.r, pl.ds(base, PAIRS), :] += high
                acc[k.c, k.r, pl.ds(base + PAIRS, PAIRS), :] += low
            return carry

        lax.fori_loop(0, CROWS // LANES, block, 0, unroll=True)

    phase("y_unpack")
    for k in colours:
        arrive(k.y_l)
        unpack(k, 0)
        arrive(k.y_r)
        unpack(k, 1)
    phase("y_unpack_o")
    for k in colours:
        arrive(k.y_o)
        unpack(k, 2)

    phase("z_pack")
    for k in colours:
        def aux(b, step, count, k=k):
            zaux[b, 2 * k.c : 2 * k.c + 1, :] = step
            for s in range(3):
                count = count + yauxr[k.c, s, b, 1:2, :]
            zaux[b, 2 * k.c + 1 : 2 * k.c + 2, :] = count

        pack(k.c, k.r, lambda zb, k=k: zsend.at[zb, k.c], aux)
    zcopies = {}
    for d in (4, 3, 5, 2, 6, 1, 7):
        to = zat(d)
        zcopies[d] = [
            remote(zaux.at[to // 2], zauxr.at[d - 1], at_z(to)),
            remote(zsend.at[to], zrecv.at[d - 1], at_z(to)),
        ]
    phase("dist1")
    c_p.wait_recv()
    distances(1, 0, 2048 // TILE)
    eye = lane_eye(LANES)
    for b in range(ROWS // LANES):
        part = pv[pl.ds(b * LANES, LANES), :].astype(jnp.float32)
        square = to_row(jnp.sum(part * part, axis=1, keepdims=True), eye)
        lanes = pl.ds(b * LANES, LANES)
        cost_ref[:, lanes] = (square + jnp.min(best[:, lanes], axis=0, keepdims=True)) * (1.0 / 1024)
    phase("z_sum")
    mine = lane_eye(OWN, lax.rem(z, 2) * OWN)
    for k in colours:
        sums = acc[k.c, k.r, pl.ds(pl.multiple_of(z * OWN, OWN), OWN), :]
        k.high, k.low = sums[:PAIRS], sums[PAIRS:]
        k.count = zaux[z // 2, 2 * k.c + 1 : 2 * k.c + 2, :]
    for d in (1, 7, 2, 6, 3, 5, 4):
        arrive(zcopies[d])
        for k in colours:
            step = to_col(zauxr[d - 1, 2 * k.c : 2 * k.c + 1, :], mine)
            high, low = decode(zrecv[d - 1, k.c], step)
            k.high, k.low = k.high + high, k.low + low
            k.count = k.count + zauxr[d - 1, 2 * k.c + 1 : 2 * k.c + 2, :]
    phase("fresh")
    for k in colours:
        count = to_col(k.count, mine)
        rows = pl.ds(pl.multiple_of((k.r * NZ + z) * OWN, OWN), OWN)
        prior = cv[0, rows, k.cols(k.f)].astype(jnp.float32)
        sums = jnp.concatenate([k.high, k.low], axis=0)
        code, step = encode(jnp.where(count > 0.5, sums / jnp.maximum(count, 1.0), prior))
        words_ref[k.c, k.f, k.r, z] = pair(code)
        steps_ref[k.c, k.f, k.r, z] = to_row(step, lane_eye(OWN))
        k.start = []
        for to in (k.ro, k.rr, k.rl):
            for ref in (steps_ref, words_ref):
                own_piece = ref.at[k.c, k.f, k.r, z]
                k.start.append(remote(own_piece, own_piece, k.at_r(to)))

    def group(k, f, zc, device):
        copies = []
        for ref in (steps_ref, words_ref):
            piece = ref.at[k.c, f, :, zc]
            copies.append(remote(piece, piece, device))
        return copies

    def hop(k, way, h, half):
        zc, device = zat(-way * (h - 1)), at_z(zat(way))
        copies = []
        if half == 0:
            piece = steps_ref.at[k.c, k.f, :, zc]
            copies.append(remote(piece, piece, device))
        piece = words_ref.at[k.c, k.f, pl.ds(half * (N // 2), N // 2), zc]
        copies.append(remote(piece, piece, device))
        k.hops[way, h, half] = copies

    def spread(k, d):
        zc = zat(d)
        k.side[d] = (group(k, k.f, zc, k.at_f(k.fr)), group(k, k.f, zc, k.at_f(k.fl)))

    def left_first(d):
        return d in (0, 1, 2, 3)

    def across(k, d):
        zc = zat(d)
        from_left, from_right = k.side[d]
        if left_first(d):
            arrive(from_left)
            k.last[d] = (group(k, k.fl, zc, k.at_f(k.fr)), from_right)
        else:
            arrive(from_right)
            k.last[d] = (group(k, k.fr, zc, k.at_f(k.fl)), from_left)

    def finish(groups):
        def block(r, carry):
            for k, f, d in groups:
                zc = zat(d)
                step = to_col(steps_ref[k.c, f, r, zc], lane_eye(OWN))
                high, low = decode(words_ref[k.c, f, r, zc], step)
                base = pl.multiple_of((r * NZ + zc) * OWN, OWN)
                out_ref[pl.ds(base, PAIRS), k.cols(f)] = high
                out_ref[pl.ds(base + PAIRS, PAIRS), k.cols(f)] = low
            return carry

        lax.fori_loop(0, N, block, 0)

    phase("g1")
    for k in colours:
        arrive(k.start)
        k.hops, k.side, k.last = {}, {}, {}
        for half in (0, 1):
            for way in (1, -1):
                hop(k, way, 1, half)
        spread(k, 0)
    rounds = ((0,), (-1, 1), (-2, 2), (-3, 3), (4,))
    for h in range(1, 7):
        if h <= 4:
            phase(f"g_z{h}")
            for k in colours:
                for half in (0, 1):
                    for way in (1, -1):
                        if h < 4 or way == (1, -1)[half]:
                            arrive(k.hops[way, h, half])
                            if h < 3 or (h == 3 and way == (1, -1)[half]):
                                hop(k, way, h + 1, half)
                for d in rounds[h]:
                    spread(k, d)
        if h <= 5:
            phase(f"g_x{h}")
            for k in colours:
                for d in rounds[h - 1]:
                    across(k, d)
        phase(f"g_f{h}")
        groups = []
        for k in colours:
            for d in rounds[h - 1] if h <= 5 else ():
                groups += [(k, k.f, d), (k, k.fl if left_first(d) else k.fr, d)]
            for d in rounds[h - 2] if h >= 2 else ():
                for copies in k.last[d]:
                    arrive(copies)
                groups += [(k, k.fo, d), (k, k.fr if left_first(d) else k.fl, d)]
        finish(groups)
    phase("w_send")
    for copy in used:
        copy.wait_send()
    phase(None)
    assert len(used) == N_COPIES, len(used)


N_COPIES = 216


def put_kernel(rows_ref, cost_ref, rows_hbm, cost_hbm, sems):
    puts = [pltpu.make_async_copy(cost_ref, cost_hbm, sems.at[N])]
    for q in range(N):
        rows = pl.ds(q * CROWS, CROWS)
        puts.append(pltpu.make_async_copy(rows_ref.at[rows], rows_hbm.at[rows], sems.at[q]))
    for put in puts:
        put.start()
    for put in puts:
        put.wait()


def shards(points, centroids, assign, keep_mask):
    vmem = pl.BlockSpec(memory_space=pltpu.VMEM)
    hbm = pl.BlockSpec(memory_space=pltpu.HBM)
    dma = pltpu.SemaphoreType.DMA
    f32, i32, bf16 = jnp.float32, jnp.int32, jnp.bfloat16
    args = (points, centroids, assign.reshape(1, ROWS), keep_mask.reshape(1, ROWS))
    rows, cost = pl.pallas_call(
        update_kernel,
        out_shape=(
            jax.ShapeDtypeStruct((2048, 1024), f32),
            jax.ShapeDtypeStruct((1, ROWS), f32),
        ),
        in_specs=[hbm] * 4,
        out_specs=(vmem, vmem),
        scratch_shapes=[
            pltpu.VMEM((2, N, N, NZ, PAIRS, LANES), i32),
            pltpu.VMEM((2, N, N, NZ, 1, LANES), f32),
            pltpu.VMEM((ROWS, 1024), bf16),
            pltpu.VMEM((2, 2048, 1024), bf16),
            pltpu.VMEM((2, 1, ROWS), i32),
            pltpu.VMEM((2 * ROWS, 2 * LANES), bf16),
            pltpu.VMEM((2, 6 * ROWS, LANES), bf16),
            pltpu.VMEM((1, 2 * ROWS), i32),
            pltpu.VMEM((2, 1, 6 * ROWS), i32),
            pltpu.VMEM((2, 2, ROWS // 2, LANES), bf16),
            pltpu.VMEM((8, ROWS), f32),
            pltpu.VMEM((2, N, CROWS, LANES), f32),
            pltpu.VMEM((2, N, CROWS, LANES), bf16),
            pltpu.VMEM((2, 3, NZ, PAIRS, LANES), i32),
            pltpu.VMEM((2, 3, N, 2, LANES), f32),
            pltpu.VMEM((2, 4, NZ, PAIRS, LANES), i32),
            pltpu.VMEM((2, 3, N, 2, LANES), f32),
            pltpu.VMEM((NZ, 2, PAIRS, LANES), i32),
            pltpu.VMEM((N, 4, LANES), f32),
            pltpu.VMEM((NZ - 1, 2, PAIRS, LANES), i32),
            pltpu.VMEM((NZ - 1, 4, LANES), f32),
            dma((N_COPIES,)), dma((N_COPIES,)), dma((6,)),
        ],
        compiler_params=pltpu.CompilerParams(
            collective_id=0, has_side_effects=True, vmem_limit_bytes=40 * 1024 * 1024
        ),
    )(*(pltpu.with_memory_space_constraint(a, pltpu.HBM) for a in args))
    new_centroids, cost = pl.pallas_call(
        put_kernel,
        out_shape=(jax.ShapeDtypeStruct((2048, 1024), f32), jax.ShapeDtypeStruct((1, ROWS), f32)),
        in_specs=[vmem] * 2,
        out_specs=(hbm, hbm),
        scratch_shapes=[dma((N + 1,))],
        compiler_params=pltpu.CompilerParams(vmem_limit_bytes=1024 * 1024),
        cost_estimate=pl.CostEstimate(flops=0, bytes_accessed=16 << 20, transcendentals=0),
    )(rows, cost)
    return new_centroids, cost.reshape(ROWS)


def solution(mesh):
    grid = Mesh(mesh.devices.reshape(NZ, N, N, 2), ("z", "y", "x", "mp"))
    rows = ("z", "y", "x", "mp")
    in_specs = (P(rows, None), P("mp", None), P(rows), P(rows))
    out_specs = (P("mp", None), P(rows))
    return jax.shard_map(shards, mesh=grid, in_specs=in_specs, out_specs=out_specs, check_vma=False)
```

```python
import jax
import jax.numpy as jnp
from jax import lax
from jax.experimental import pallas as pl
from jax.experimental.pallas import tpu as pltpu
from jax.sharding import Mesh
from jax.sharding import PartitionSpec as P

STEPS = 32000.0
TINY = 2.0**-100
N, NZ = 4, 8
LANES = 128
CROWS = 512
OWN = 64
PAIRS = OWN // 2
TILE = 256
ROWS = 512
MESH_ID = pl.DeviceIdType.MESH


def encode(v):
    top = jnp.maximum(jnp.max(jnp.abs(v), axis=1, keepdims=True), TINY)
    code = jnp.floor(v * (STEPS / top) + 0.5).astype(jnp.int32)
    return code, top * (1.0 / STEPS)


def pair(code):
    return (code[:PAIRS] << 16) | (code[PAIRS:] & 0xFFFF)


def decode(words, step):
    high = (words >> 16).astype(jnp.float32)
    low = ((words << 16) >> 16).astype(jnp.float32)
    return high * step[:PAIRS], low * step[PAIRS:]


def lane_eye(rows, shift=0):
    at_row = lax.broadcasted_iota(jnp.int32, (rows, LANES), 0)
    at_lane = lax.broadcasted_iota(jnp.int32, (rows, LANES), 1)
    return at_lane == at_row + shift


def to_row(col, eye):
    return jnp.sum(jnp.where(eye, col, 0.0), axis=0, keepdims=True)


def to_col(row, eye):
    return jnp.sum(jnp.where(eye, row, 0.0), axis=1, keepdims=True)


def update_kernel(
    p_hbm, c_hbm, assign_hbm, keep_hbm, out_ref, cost_ref,
    words_ref, steps_ref,
    pv, cv, idv, near0, near, ids0, ids, relay, best, acc, cnt,
    ysend, yaux, yrecv, yauxr, zsend, zaux, zrecv, zauxr,
    send_sem, recv_sem, local_sem,
):
    z, y, x, m = (lax.axis_index(n) for n in ("z", "y", "x", "mp"))
    zat = lambda d: lax.rem(z + d + NZ, NZ)
    used = []
    scopes = []

    def phase(name):
        if scopes:
            scopes.pop().__exit__(None, None, None)
        if name:
            scopes.append(jax.named_scope(name))
            scopes[-1].__enter__()

    def remote(src, dst, device):
        k = len(used)
        copy = pltpu.make_async_remote_copy(
            src_ref=src, dst_ref=dst, send_sem=send_sem.at[k], recv_sem=recv_sem.at[k],
            device_id=device, device_id_type=MESH_ID,
        )
        copy.start()
        used.append(copy)
        return copy

    def arrive(copies):
        for copy in copies:
            copy.wait_recv()

    at_x = lambda to: (z, y, to, m)
    at_y = lambda to: (z, to, x, m)
    at_z = lambda to: (to, y, x, m)
    partner = (z, y, x, 1 - m)

    class Colour:
        def __init__(self, c, first, second, at_first, at_second):
            self.c, self.f, self.r = c, first, second
            self.fr, self.fl, self.fo = (lax.rem(first + d, N) for d in (1, 3, 2))
            self.rr, self.rl, self.ro = (lax.rem(second + d, N) for d in (1, 3, 2))
            self.at_f, self.at_r = at_first, at_second

        def cols(self, f):
            return pl.ds(pl.multiple_of(self.c * 512 + f * LANES, LANES), LANES)

    colours = (Colour(0, x, y, at_x, at_y), Colour(1, y, x, at_y, at_x))

    phase("enter")
    loads = [
        pltpu.make_async_copy(p_hbm, pv, local_sem.at[0]),
        pltpu.make_async_copy(assign_hbm, idv.at[0], local_sem.at[1]),
        pltpu.make_async_copy(keep_hbm, idv.at[1], local_sem.at[2]),
    ]
    load_c = pltpu.make_async_copy(c_hbm, cv.at[0], local_sem.at[3])
    for copy in loads + [load_c]:
        copy.start()

    peers = [partner] + [at_z(zat(d)) for d in range(1, NZ)]
    for k in colours:
        peers += [k.at_f(k.fr), k.at_f(k.fl), k.at_f(k.fo)]
    barrier = pltpu.get_barrier_semaphore()
    for peer in peers:
        pl.semaphore_signal(barrier, inc=1, device_id=peer, device_id_type=MESH_ID)
    for copy in loads:
        copy.wait()
    ids0[:, :ROWS] = jnp.where(idv[1] > 0, idv[0], -1)
    best[...] = jnp.full(best.shape, jnp.inf, jnp.float32)
    pl.semaphore_wait(barrier, len(peers))

    phase("send_p")

    def slot(s):
        return pl.ds((s - 2) * ROWS, ROWS)

    lo, hi = pl.ds(0, ROWS // 2), pl.ds(ROWS // 2, ROWS // 2)
    mine_ids = ids0.at[:, pl.ds(0, ROWS)]
    for k in colours:
        k.relay_l = remote(pv.at[lo, k.cols(k.fo)], relay.at[k.c, 0], k.at_f(k.fr))
        k.relay_r = remote(pv.at[hi, k.cols(k.fo)], relay.at[k.c, 1], k.at_f(k.fl))
    own = []
    from_p = [remote(mine_ids, ids0.at[:, pl.ds(ROWS, ROWS)], partner)]
    for k in colours:
        lanes = pl.ds(k.c * LANES, LANES)
        own.append(
            pltpu.make_async_copy(pv.at[:, k.cols(k.f)], near0.at[pl.ds(0, ROWS), lanes], local_sem.at[4 + k.c])
        )
        own[-1].start()
        from_p.append(remote(pv.at[:, k.cols(k.f)], near0.at[pl.ds(ROWS, ROWS), lanes], partner))
    for k in colours:
        k.from_l = [
            remote(mine_ids, ids.at[k.c, :, slot(2)], k.at_f(k.fr)),
            remote(pv.at[:, k.cols(k.fr)], near.at[k.c, slot(2)], k.at_f(k.fr)),
        ]
        k.from_r = [
            remote(mine_ids, ids.at[k.c, :, slot(3)], k.at_f(k.fl)),
            remote(pv.at[:, k.cols(k.fl)], near.at[k.c, slot(3)], k.at_f(k.fl)),
        ]
        k.from_o = [remote(mine_ids, ids.at[k.c, :, slot(6)], k.at_f(k.fo))]
    c_p = remote(c_hbm, cv.at[1], partner)

    def distances(s, first, count):
        def tile(t, carry):
            part = cv[s, pl.ds(pl.multiple_of(t * TILE, TILE), TILE), :]
            inner = lax.dot_general(
                part, pv[...], (((1,), (1,)), ((), ())), preferred_element_type=jnp.float32
            )
            wide = part.astype(jnp.float32)
            square = jnp.sum(wide * wide, axis=1, keepdims=True)
            dist = square - 2.0 * inner
            low = jnp.min(dist.reshape(TILE // 8, 8, ROWS), axis=0)
            best[...] = jnp.minimum(best[...], low)
            return carry

        lax.fori_loop(first, first + count, tile, 0)

    def hits(id_row, base):
        local = id_row - base
        local = jnp.where((local >= 0) & (local < TILE), local, -1).astype(jnp.float32)
        width = id_row.shape[1]
        local = jnp.broadcast_to(local, (16, width)).astype(jnp.bfloat16)
        at = lax.broadcasted_iota(jnp.int32, (TILE, LANES), 0).astype(jnp.float32).astype(jnp.bfloat16)
        at = at.reshape(TILE // 16, 16, LANES)
        one, zero = jnp.ones((), jnp.bfloat16), jnp.zeros((), jnp.bfloat16)
        parts = [
            jnp.where(at == local[None, :, i * LANES : (i + 1) * LANES], one, zero).reshape(TILE, LANES)
            for i in range(width // LANES)
        ]
        count = parts[0]
        for part in parts[1:]:
            count = count + part
        return jnp.concatenate(parts, axis=1), count

    def hits_chunk(id_row, base):
        low, count_low = hits(id_row, base)
        high, count_high = hits(id_row, base + TILE)
        return jnp.concatenate([low, high], axis=0), jnp.concatenate([count_low, count_high], axis=0)

    def accumulate(c, first, count, q):
        where = pl.ds((first - 2) * ROWS, count * ROWS)
        hit, number = hits_chunk(ids[c, :, where], m * 2048 + q * CROWS)
        acc[c, q] += jnp.dot(hit, near[c, where, :], preferred_element_type=jnp.float32)
        cnt[c, q] += number

    def accumulate_all(c, first, count):
        def body(q, carry):
            accumulate(c, first, count, q)
            return carry

        lax.fori_loop(0, N, body, 0)

    def accumulate_own():
        def body(q, carry):
            hit, count = hits_chunk(ids0[...], m * 2048 + q * CROWS)
            part = jnp.dot(hit, near0[...], preferred_element_type=jnp.float32)
            for c in range(2):
                acc[c, q] = part[:, c * LANES : (c + 1) * LANES]
                cnt[c, q] = count
            return carry

        lax.fori_loop(0, N, body, 0)

    phase("dist0a")
    load_c.wait()
    distances(0, 0, 4)
    phase("w_own")
    for copy in own:
        copy.wait()
    arrive(from_p)
    phase("acc0")
    accumulate_own()
    phase("w_relay")
    for k in colours:
        k.relay_l.wait_recv()
        k.from_o.append(remote(relay.at[k.c, 0], near.at[k.c, pl.ds(4 * ROWS, ROWS // 2)], k.at_f(k.fr)))
        k.relay_r.wait_recv()
        k.from_o.append(remote(relay.at[k.c, 1], near.at[k.c, pl.ds(4 * ROWS + ROWS // 2, ROWS // 2)], k.at_f(k.fl)))
    phase("dist0b")
    distances(0, 4, 4)

    def to_partner(k, source, target):
        return [
            remote(near.at[k.c, slot(source)], near.at[k.c, slot(target)], partner),
            remote(ids.at[k.c, :, slot(source)], ids.at[k.c, :, slot(target)], partner),
        ]

    phase("w_lr")
    for k in colours:
        arrive(k.from_l)
        k.two = to_partner(k, 2, 4)
        arrive(k.from_r)
        k.two += to_partner(k, 3, 5)
    phase("acc1")
    accumulate_all(0, 2, 2)
    phase("w_o")
    for k in colours:
        arrive(k.from_o)
        k.three = to_partner(k, 6, 7)
    phase("w_plr")
    for k in colours:
        arrive(k.two)
    phase("acc2")
    accumulate_all(1, 2, 4)
    phase("w_po")
    for k in colours:
        arrive(k.three)
    colours[0].rest, colours[1].rest = (4, 4), (6, 2)

    def pack(c, q, words, aux):
        def block(b, carry):
            eye = lane_eye(LANES)
            rows = pl.ds(pl.multiple_of(b * LANES, LANES), LANES)
            code, step = encode(acc[c, q, rows, :])
            for j in range(2):
                words(2 * b + j)[...] = pair(code[j * OWN : (j + 1) * OWN])
            count = jnp.sum(cnt[c, q, rows, :].astype(jnp.float32), axis=1, keepdims=True)
            aux(b, to_row(step, eye), to_row(count, eye))
            return carry

        lax.fori_loop(0, CROWS // LANES, block, 0, unroll=True)

    def pack_y(k, q, s):
        def aux(b, step, count):
            yaux[k.c, s, b, 0:1, :] = step
            yaux[k.c, s, b, 1:2, :] = count

        accumulate(k.c, *k.rest, q)
        pack(k.c, q, lambda zb: ysend.at[k.c, s, zb], aux)

    h0, h1 = pl.ds(0, NZ // 2), pl.ds(NZ // 2, NZ // 2)
    phase("y_pack")
    for k in colours:
        pack_y(k, k.ro, 2)
        k.yrelay_l = remote(ysend.at[k.c, 2, h0], yrecv.at[k.c, 3, h0], k.at_r(k.rr))
        k.yrelay_r = remote(ysend.at[k.c, 2, h1], yrecv.at[k.c, 3, h1], k.at_r(k.rl))
        k.y_o = [remote(yaux.at[k.c, 2], yauxr.at[k.c, 2], k.at_r(k.ro))]
    for k in colours:
        pack_y(k, k.rr, 0)
        k.y_l = [
            remote(yaux.at[k.c, 0], yauxr.at[k.c, 0], k.at_r(k.rr)),
            remote(ysend.at[k.c, 0], yrecv.at[k.c, 0], k.at_r(k.rr)),
        ]
        pack_y(k, k.rl, 1)
        k.y_r = [
            remote(yaux.at[k.c, 1], yauxr.at[k.c, 1], k.at_r(k.rl)),
            remote(ysend.at[k.c, 1], yrecv.at[k.c, 1], k.at_r(k.rl)),
        ]
    phase("y_relay")
    for k in colours:
        k.yrelay_l.wait_recv()
        k.y_o.append(remote(yrecv.at[k.c, 3, h0], yrecv.at[k.c, 2, h0], k.at_r(k.rr)))
        k.yrelay_r.wait_recv()
        k.y_o.append(remote(yrecv.at[k.c, 3, h1], yrecv.at[k.c, 2, h1], k.at_r(k.rl)))
    for k in colours:
        accumulate(k.c, *k.rest, k.r)

    def unpack(k, s):
        def block(b, carry):
            step = to_col(yauxr[k.c, s, b, 0:1, :], lane_eye(LANES))
            for j in range(2):
                high, low = decode(yrecv[k.c, s, 2 * b + j], step[j * OWN : (j + 1) * OWN])
                base = pl.multiple_of(b * LANES, LANES) + j * OWN
                acc[k.c, k.r, pl.ds(base, PAIRS), :] += high
                acc[k.c, k.r, pl.ds(base + PAIRS, PAIRS), :] += low
            return carry

        lax.fori_loop(0, CROWS // LANES, block, 0, unroll=True)

    phase("y_unpack")
    for k in colours:
        arrive(k.y_l)
        unpack(k, 0)
        arrive(k.y_r)
        unpack(k, 1)
    phase("y_unpack_o")
    for k in colours:
        arrive(k.y_o)
        unpack(k, 2)

    phase("z_pack")
    for k in colours:
        def aux(b, step, count, k=k):
            zaux[b, 2 * k.c : 2 * k.c + 1, :] = step
            for s in range(3):
                count = count + yauxr[k.c, s, b, 1:2, :]
            zaux[b, 2 * k.c + 1 : 2 * k.c + 2, :] = count

        pack(k.c, k.r, lambda zb, k=k: zsend.at[zb, k.c], aux)
    zcopies = {}
    for d in (4, 3, 5, 2, 6, 1, 7):
        to = zat(d)
        zcopies[d] = [
            remote(zaux.at[to // 2], zauxr.at[d - 1], at_z(to)),
            remote(zsend.at[to], zrecv.at[d - 1], at_z(to)),
        ]
    phase("dist1")
    c_p.wait_recv()
    distances(1, 0, 2048 // TILE)
    eye = lane_eye(LANES)
    for b in range(ROWS // LANES):
        part = pv[pl.ds(b * LANES, LANES), :].astype(jnp.float32)
        square = to_row(jnp.sum(part * part, axis=1, keepdims=True), eye)
        lanes = pl.ds(b * LANES, LANES)
        cost_ref[:, lanes] = (square + jnp.min(best[:, lanes], axis=0, keepdims=True)) * (1.0 / 1024)
    phase("z_sum")
    mine = lane_eye(OWN, lax.rem(z, 2) * OWN)
    for k in colours:
        sums = acc[k.c, k.r, pl.ds(pl.multiple_of(z * OWN, OWN), OWN), :]
        k.high, k.low = sums[:PAIRS], sums[PAIRS:]
        k.count = zaux[z // 2, 2 * k.c + 1 : 2 * k.c + 2, :]
    for d in (1, 7, 2, 6, 3, 5, 4):
        arrive(zcopies[d])
        for k in colours:
            step = to_col(zauxr[d - 1, 2 * k.c : 2 * k.c + 1, :], mine)
            high, low = decode(zrecv[d - 1, k.c], step)
            k.high, k.low = k.high + high, k.low + low
            k.count = k.count + zauxr[d - 1, 2 * k.c + 1 : 2 * k.c + 2, :]
    phase("fresh")
    for k in colours:
        count = to_col(k.count, mine)
        rows = pl.ds(pl.multiple_of((k.r * NZ + z) * OWN, OWN), OWN)
        prior = cv[0, rows, k.cols(k.f)].astype(jnp.float32)
        sums = jnp.concatenate([k.high, k.low], axis=0)
        code, step = encode(jnp.where(count > 0.5, sums / jnp.maximum(count, 1.0), prior))
        words_ref[k.c, k.f, 0, z] = pair(code)
        steps_ref[k.c, k.f, 0, z] = to_row(step, lane_eye(OWN))

    parts = (pl.ds(0, 1), pl.ds(1, N - 1))

    def hop(k, way, h, s):
        zc, device = zat(-way * (h - 1)), at_z(zat(way))
        piece = words_ref.at[k.c, k.f, s, zc]
        copies = [remote(piece, piece, device)]
        if s == 2:
            piece = steps_ref.at[k.c, k.f, :, zc]
            copies.append(remote(piece, piece, device))
        k.hops[way, h, s] = copies

    def group(k, f, zc, part, device):
        piece = words_ref.at[k.c, f, parts[part], zc]
        copies = [remote(piece, piece, device)]
        if part:
            piece = steps_ref.at[k.c, f, :, zc]
            copies.append(remote(piece, piece, device))
        return copies

    def spread(k, d, part):
        zc = zat(d)
        k.side[d, part] = (group(k, k.f, zc, part, k.at_f(k.fr)), group(k, k.f, zc, part, k.at_f(k.fl)))
        if d in (-3, 3, 4):
            k.far[d, part] = group(k, k.f, zc, part, k.at_f(k.fo))

    def left_first(d):
        return d in (0, 1, 2, 3)

    def across(k, d, part):
        zc = zat(d)
        from_left, from_right = k.side[d, part]
        if left_first(d):
            arrive(from_left)
            k.last[d, part] = group(k, k.fl, zc, part, k.at_f(k.fr)) + from_right
        else:
            arrive(from_right)
            k.last[d, part] = group(k, k.fr, zc, part, k.at_f(k.fl)) + from_left

    def finish(groups):
        def block(s, carry):
            for k, f, d in groups:
                zc = zat(d)
                step = to_col(steps_ref[k.c, f, s, zc], lane_eye(OWN))
                high, low = decode(words_ref[k.c, f, s, zc], step)
                base = pl.multiple_of((lax.rem(k.r + s, N) * NZ + zc) * OWN, OWN)
                out_ref[pl.ds(base, PAIRS), k.cols(f)] = high
                out_ref[pl.ds(base + PAIRS, PAIRS), k.cols(f)] = low
            return carry

        lax.fori_loop(0, N, block, 0)

    def own_done(*ds):
        return [(k, k.f, d) for k in colours for d in ds]

    def first_done(*ds):
        return [(k, k.fl if left_first(d) else k.fr, d) for k in colours for d in ds]

    def last_done(*ds):
        for k in colours:
            for d in ds:
                arrive(k.last[d, 0] + k.last[d, 1])
        return [(k, f, d) for k in colours for d in ds for f in (k.fo, k.fr if left_first(d) else k.fl)]

    def far_way(k, s):
        return 1 if (s < 2) == (k.c == 0) else -1

    def z_round(h, chunks, part):
        phase(f"g_z{h}p{part}")
        for k in colours:
            for s in chunks:
                for way in (1, -1):
                    if h < 4 or way == far_way(k, s):
                        arrive(k.hops[way, h, s])
                        if h < 3 or (h == 3 and way == far_way(k, s)):
                            hop(k, way, h + 1, s)
            for d in ((-h, h) if h < 4 else (4,)):
                spread(k, d, part)

    def x_round(part, *ds):
        phase("g_x%d" % part)
        for k in colours:
            for d in ds:
                across(k, d, part)

    def hop_opposite(way, h):
        zc, device = zat(-way * (h - 1)), at_z(zat(way))
        for k in colours:
            k.opposite[way, h] = group(k, k.fo, zc, 0, device) + group(k, k.fo, zc, 1, device)

    def opposite_done(h):
        for k in colours:
            arrive(k.opposite[1, h] + k.opposite[-1, h])
        return [(k, k.fo, d) for k in colours for d in (-h, h)]

    def sides_done(*ds):
        for k in colours:
            for d in ds:
                for part in (0, 1):
                    arrive(k.side[d, part][0] + k.side[d, part][1])
        return [(k, f, d) for k in colours for d in ds for f in (k.fl, k.fr)]

    phase("g_0")
    for k in colours:
        k.hops, k.side, k.last, k.start, k.opposite, k.far = {}, {}, {}, {}, {}, {}
        for s, to in ((2, k.ro), (3, k.rr), (1, k.rl)):
            k.start[s] = [
                remote(ref.at[k.c, k.f, 0, z], ref.at[k.c, k.f, s, z], k.at_r(to)) for ref in (words_ref, steps_ref)
            ]
        hop(k, 1, 1, 0)
        hop(k, -1, 1, 0)
        spread(k, 0, 0)
    z_round(1, (0,), 0)
    phase("g_1")
    for k in colours:
        for s in (3, 1, 2):
            arrive(k.start[s])
            hop(k, 1, 1, s)
            hop(k, -1, 1, s)
        spread(k, 0, 1)
    x_round(0, 0)
    z_round(2, (0,), 0)
    z_round(1, (3, 1, 2), 1)
    x_round(1, 0)
    z_round(3, (0,), 0)
    phase("g_f1")
    finish(own_done(0, -1, 1) + first_done(0))
    z_round(2, (3, 1, 2), 1)
    phase("g_o1")
    done = last_done(0)
    hop_opposite(1, 1)
    hop_opposite(-1, 1)
    z_round(4, (0,), 0)
    x_round(0, -2, 2)
    phase("g_f2")
    finish(own_done(-2, 2) + done + sides_done(-1, 1))
    z_round(3, (3, 1, 2), 1)
    x_round(1, -2, 2)
    phase("g_f3")
    finish(own_done(-3, 3) + first_done(-2, 2))
    z_round(4, (3, 1, 2), 1)
    phase("g_f4")
    finish(own_done(4) + opposite_done(1) + last_done(-2, 2))
    phase("g_f5")
    finish(sides_done(-3, 3))
    phase("g_f6")
    for k in colours:
        for d in (-3, 3, 4):
            arrive(k.far[d, 0] + k.far[d, 1])
    finish([(k, k.fo, d) for k in colours for d in (-3, 3, 4)] + sides_done(4))
    phase("w_send")
    for copy in used:
        copy.wait_send()
    phase(None)
    assert len(used) == N_COPIES, len(used)


N_COPIES = 292


def put_kernel(rows_ref, cost_ref, rows_hbm, cost_hbm, sems):
    puts = [pltpu.make_async_copy(cost_ref, cost_hbm, sems.at[N])]
    for q in range(N):
        rows = pl.ds(q * CROWS, CROWS)
        puts.append(pltpu.make_async_copy(rows_ref.at[rows], rows_hbm.at[rows], sems.at[q]))
    for put in puts:
        put.start()
    for put in puts:
        put.wait()


def shards(points, centroids, assign, keep_mask):
    vmem = pl.BlockSpec(memory_space=pltpu.VMEM)
    hbm = pl.BlockSpec(memory_space=pltpu.HBM)
    dma = pltpu.SemaphoreType.DMA
    f32, i32, bf16 = jnp.float32, jnp.int32, jnp.bfloat16
    args = (points, centroids, assign.reshape(1, ROWS), keep_mask.reshape(1, ROWS))
    rows, cost = pl.pallas_call(
        update_kernel,
        out_shape=(
            jax.ShapeDtypeStruct((2048, 1024), f32),
            jax.ShapeDtypeStruct((1, ROWS), f32),
        ),
        in_specs=[hbm] * 4,
        out_specs=(vmem, vmem),
        scratch_shapes=[
            pltpu.VMEM((2, N, N, NZ, PAIRS, LANES), i32),
            pltpu.VMEM((2, N, N, NZ, 1, LANES), f32),
            pltpu.VMEM((ROWS, 1024), bf16),
            pltpu.VMEM((2, 2048, 1024), bf16),
            pltpu.VMEM((2, 1, ROWS), i32),
            pltpu.VMEM((2 * ROWS, 2 * LANES), bf16),
            pltpu.VMEM((2, 6 * ROWS, LANES), bf16),
            pltpu.VMEM((1, 2 * ROWS), i32),
            pltpu.VMEM((2, 1, 6 * ROWS), i32),
            pltpu.VMEM((2, 2, ROWS // 2, LANES), bf16),
            pltpu.VMEM((8, ROWS), f32),
            pltpu.VMEM((2, N, CROWS, LANES), f32),
            pltpu.VMEM((2, N, CROWS, LANES), bf16),
            pltpu.VMEM((2, 3, NZ, PAIRS, LANES), i32),
            pltpu.VMEM((2, 3, N, 2, LANES), f32),
            pltpu.VMEM((2, 4, NZ, PAIRS, LANES), i32),
            pltpu.VMEM((2, 3, N, 2, LANES), f32),
            pltpu.VMEM((NZ, 2, PAIRS, LANES), i32),
            pltpu.VMEM((N, 4, LANES), f32),
            pltpu.VMEM((NZ - 1, 2, PAIRS, LANES), i32),
            pltpu.VMEM((NZ - 1, 4, LANES), f32),
            dma((N_COPIES,)), dma((N_COPIES,)), dma((6,)),
        ],
        compiler_params=pltpu.CompilerParams(
            collective_id=0, has_side_effects=True, vmem_limit_bytes=40 * 1024 * 1024
        ),
    )(*(pltpu.with_memory_space_constraint(a, pltpu.HBM) for a in args))
    new_centroids, cost = pl.pallas_call(
        put_kernel,
        out_shape=(jax.ShapeDtypeStruct((2048, 1024), f32), jax.ShapeDtypeStruct((1, ROWS), f32)),
        in_specs=[vmem] * 2,
        out_specs=(hbm, hbm),
        scratch_shapes=[dma((N + 1,))],
        compiler_params=pltpu.CompilerParams(vmem_limit_bytes=1024 * 1024),
        cost_estimate=pl.CostEstimate(flops=0, bytes_accessed=16 << 20, transcendentals=0),
    )(rows, cost)
    return new_centroids, cost.reshape(ROWS)


def solution(mesh):
    grid = Mesh(mesh.devices.reshape(NZ, N, N, 2), ("z", "y", "x", "mp"))
    rows = ("z", "y", "x", "mp")
    in_specs = (P(rows, None), P("mp", None), P(rows), P(rows))
    out_specs = (P("mp", None), P(rows))
    return jax.shard_map(shards, mesh=grid, in_specs=in_specs, out_specs=out_specs, check_vma=False)
```

```python
import jax
import jax.numpy as jnp
from jax import lax
from jax.experimental import pallas as pl
from jax.experimental.pallas import tpu as pltpu
from jax.sharding import Mesh
from jax.sharding import PartitionSpec as P

STEPS = 32000.0
TINY = 2.0**-100
N, NZ = 4, 8
LANES = 128
CROWS = 512
HROWS = CROWS // 2
OWN = HROWS // NZ
PAIRS = OWN // 2
TILE = 256
ROWS = 512
MESH_ID = pl.DeviceIdType.MESH


def encode(v):
    top = jnp.maximum(jnp.max(jnp.abs(v), axis=1, keepdims=True), TINY)
    code = jnp.floor(v * (STEPS / top) + 0.5).astype(jnp.int32)
    return code, top * (1.0 / STEPS)


def pair(code):
    return (code[:PAIRS] << 16) | (code[PAIRS:] & 0xFFFF)


def decode(words, step):
    high = (words >> 16).astype(jnp.float32)
    low = ((words << 16) >> 16).astype(jnp.float32)
    return high * step[:PAIRS], low * step[PAIRS:]


def lane_eye(rows, shift=0):
    at_row = lax.broadcasted_iota(jnp.int32, (rows, LANES), 0)
    at_lane = lax.broadcasted_iota(jnp.int32, (rows, LANES), 1)
    return at_lane == at_row + shift


def to_row(col, eye):
    return jnp.sum(jnp.where(eye, col, 0.0), axis=0, keepdims=True)


def to_col(row, eye):
    return jnp.sum(jnp.where(eye, row, 0.0), axis=1, keepdims=True)


def update_kernel(
    p_hbm, c_hbm, assign_hbm, keep_hbm, out_ref, cost_ref,
    words_ref, steps_ref,
    pv, cv, idv, near0, near, ids0, ids, relay, best, acc, cnt,
    ysend, yaux, yrecv, yauxr, zsend, zaux, zrecv, zauxr,
    send_sem, recv_sem, local_sem,
):
    z, y, x, m = (lax.axis_index(n) for n in ("z", "y", "x", "mp"))
    zat = lambda d: lax.rem(z + d + NZ, NZ)
    used = []
    scopes = []

    def phase(name):
        if scopes:
            scopes.pop().__exit__(None, None, None)
        if name:
            scopes.append(jax.named_scope(name))
            scopes[-1].__enter__()

    def remote(src, dst, device):
        k = len(used)
        copy = pltpu.make_async_remote_copy(
            src_ref=src, dst_ref=dst, send_sem=send_sem.at[k], recv_sem=recv_sem.at[k],
            device_id=device, device_id_type=MESH_ID,
        )
        copy.start()
        used.append(copy)
        return copy

    def arrive(copies):
        for copy in copies:
            copy.wait_recv()

    at_x = lambda to: (z, y, to, m)
    at_y = lambda to: (z, to, x, m)
    at_z = lambda to: (to, y, x, m)
    partner = (z, y, x, 1 - m)

    class Colour:
        def __init__(self, c, first, second, at_first, at_second, at_second_z):
            self.c, self.f, self.r = c, first, second
            self.fr, self.fl, self.fo = (lax.rem(first + d, N) for d in (1, 3, 2))
            self.rr, self.rl, self.ro = (lax.rem(second + d, N) for d in (1, 3, 2))
            self.at_f, self.at_r, self.at_rz = at_first, at_second, at_second_z

        def cols(self, f):
            return pl.ds(pl.multiple_of(self.c * 512 + f * LANES, LANES), LANES)

    at_xz = lambda to, to_z: (to_z, y, to, m)
    at_yz = lambda to, to_z: (to_z, to, x, m)
    colours = (Colour(0, x, y, at_x, at_y, at_yz), Colour(1, y, x, at_y, at_x, at_xz))

    phase("enter")
    loads = [
        pltpu.make_async_copy(p_hbm, pv, local_sem.at[0]),
        pltpu.make_async_copy(assign_hbm, idv.at[0], local_sem.at[1]),
        pltpu.make_async_copy(keep_hbm, idv.at[1], local_sem.at[2]),
    ]
    load_c = pltpu.make_async_copy(c_hbm, cv.at[0], local_sem.at[3])
    for copy in loads + [load_c]:
        copy.start()

    peers = [partner] + [at_z(zat(d)) for d in range(1, NZ)]
    for k in colours:
        peers += [k.at_f(k.fr), k.at_f(k.fl), k.at_f(k.fo)]
        peers += [k.at_rz(to, zat(d)) for to in (k.rr, k.rl, k.ro) for d in (1, -1)]
    barrier = pltpu.get_barrier_semaphore()
    for peer in peers:
        pl.semaphore_signal(barrier, inc=1, device_id=peer, device_id_type=MESH_ID)
    for copy in loads:
        copy.wait()
    ids0[:, :ROWS] = jnp.where(idv[1] > 0, idv[0], -1)
    best[...] = jnp.full(best.shape, jnp.inf, jnp.float32)
    pl.semaphore_wait(barrier, len(peers))

    phase("send_p")

    def slot(s):
        return pl.ds((s - 2) * ROWS, ROWS)

    lo, hi = pl.ds(0, ROWS // 2), pl.ds(ROWS // 2, ROWS // 2)
    mine_ids = ids0.at[:, pl.ds(0, ROWS)]
    for k in colours:
        k.relay_l = remote(pv.at[lo, k.cols(k.fo)], relay.at[k.c, 0], k.at_f(k.fr))
        k.relay_r = remote(pv.at[hi, k.cols(k.fo)], relay.at[k.c, 1], k.at_f(k.fl))
    own = []
    from_p = [remote(mine_ids, ids0.at[:, pl.ds(ROWS, ROWS)], partner)]
    for k in colours:
        lanes = pl.ds(k.c * LANES, LANES)
        own.append(
            pltpu.make_async_copy(pv.at[:, k.cols(k.f)], near0.at[pl.ds(0, ROWS), lanes], local_sem.at[4 + k.c])
        )
        own[-1].start()
        from_p.append(remote(pv.at[:, k.cols(k.f)], near0.at[pl.ds(ROWS, ROWS), lanes], partner))
    for k in colours:
        k.from_l = [
            remote(mine_ids, ids.at[k.c, :, slot(2)], k.at_f(k.fr)),
            remote(pv.at[:, k.cols(k.fr)], near.at[k.c, slot(2)], k.at_f(k.fr)),
        ]
        k.from_r = [
            remote(mine_ids, ids.at[k.c, :, slot(3)], k.at_f(k.fl)),
            remote(pv.at[:, k.cols(k.fl)], near.at[k.c, slot(3)], k.at_f(k.fl)),
        ]
        k.from_o = [remote(mine_ids, ids.at[k.c, :, slot(6)], k.at_f(k.fo))]
    c_p = remote(c_hbm, cv.at[1], partner)

    def distances(s, first, count):
        def tile(t, carry):
            part = cv[s, pl.ds(pl.multiple_of(t * TILE, TILE), TILE), :]
            inner = lax.dot_general(
                part, pv[...], (((1,), (1,)), ((), ())), preferred_element_type=jnp.float32
            )
            wide = part.astype(jnp.float32)
            square = jnp.sum(wide * wide, axis=1, keepdims=True)
            dist = square - 2.0 * inner
            low = jnp.min(dist.reshape(TILE // 8, 8, ROWS), axis=0)
            best[...] = jnp.minimum(best[...], low)
            return carry

        lax.fori_loop(first, first + count, tile, 0)

    def hits(id_row, base):
        local = id_row - base
        local = jnp.where((local >= 0) & (local < TILE), local, -1).astype(jnp.float32)
        width = id_row.shape[1]
        local = jnp.broadcast_to(local, (16, width)).astype(jnp.bfloat16)
        at = lax.broadcasted_iota(jnp.int32, (TILE, LANES), 0).astype(jnp.float32).astype(jnp.bfloat16)
        at = at.reshape(TILE // 16, 16, LANES)
        one, zero = jnp.ones((), jnp.bfloat16), jnp.zeros((), jnp.bfloat16)
        parts = [
            jnp.where(at == local[None, :, i * LANES : (i + 1) * LANES], one, zero).reshape(TILE, LANES)
            for i in range(width // LANES)
        ]
        count = parts[0]
        for part in parts[1:]:
            count = count + part
        return jnp.concatenate(parts, axis=1), count

    def hits_chunk(id_row, base):
        low, count_low = hits(id_row, base)
        high, count_high = hits(id_row, base + TILE)
        return jnp.concatenate([low, high], axis=0), jnp.concatenate([count_low, count_high], axis=0)

    def accumulate(c, first, count, q):
        where = pl.ds((first - 2) * ROWS, count * ROWS)
        hit, number = hits_chunk(ids[c, :, where], m * 2048 + q * CROWS)
        part = jnp.dot(hit, near[c, where, :], preferred_element_type=jnp.float32)
        acc[c, q] += part.reshape(2, HROWS, LANES)
        cnt[c, q] += number.reshape(2, HROWS, LANES)

    def accumulate_others(k, first, count):
        def body(j, carry):
            accumulate(k.c, first, count, lax.rem(k.r + 1 + j, N))
            return carry

        lax.fori_loop(0, N - 1, body, 0)

    def accumulate_own():
        def body(q, carry):
            hit, count = hits_chunk(ids0[...], m * 2048 + q * CROWS)
            part = jnp.dot(hit, near0[...], preferred_element_type=jnp.float32)
            for c in range(2):
                acc[c, q] = part[:, c * LANES : (c + 1) * LANES].reshape(2, HROWS, LANES)
                cnt[c, q] = count.reshape(2, HROWS, LANES)
            return carry

        lax.fori_loop(0, N, body, 0)

    phase("dist0a")
    load_c.wait()
    distances(0, 0, 4)
    phase("w_own")
    for copy in own:
        copy.wait()
    arrive(from_p)
    phase("acc0")
    accumulate_own()
    phase("w_relay")
    for k in colours:
        k.relay_l.wait_recv()
        k.from_o.append(remote(relay.at[k.c, 0], near.at[k.c, pl.ds(4 * ROWS, ROWS // 2)], k.at_f(k.fr)))
        k.relay_r.wait_recv()
        k.from_o.append(remote(relay.at[k.c, 1], near.at[k.c, pl.ds(4 * ROWS + ROWS // 2, ROWS // 2)], k.at_f(k.fl)))
    phase("dist0b")
    distances(0, 4, 4)

    def to_partner(k, source, target):
        return [
            remote(near.at[k.c, slot(source)], near.at[k.c, slot(target)], partner),
            remote(ids.at[k.c, :, slot(source)], ids.at[k.c, :, slot(target)], partner),
        ]

    phase("w_lr")
    for k in colours:
        arrive(k.from_l)
        k.two = to_partner(k, 2, 4)
        arrive(k.from_r)
        k.two += to_partner(k, 3, 5)
    phase("acc1")
    accumulate_others(colours[0], 2, 2)
    phase("w_o")
    for k in colours:
        arrive(k.from_o)
        k.three = to_partner(k, 6, 7)
    phase("w_plr")
    for k in colours:
        arrive(k.two)
    phase("acc2")
    accumulate_others(colours[1], 2, 4)
    phase("w_po")
    for k in colours:
        arrive(k.three)
    colours[0].rest, colours[1].rest = (4, 4), (6, 2)

    def pack(c, q, h, words, aux):
        for b in range(HROWS // LANES):
            eye = lane_eye(LANES)
            rows = pl.ds(b * LANES, LANES)
            code, step = encode(acc[c, q, h, rows, :])
            for j in range(LANES // OWN):
                words(b * (LANES // OWN) + j)[...] = pair(code[j * OWN : (j + 1) * OWN])
            count = jnp.sum(cnt[c, q, h, rows, :].astype(jnp.float32), axis=1, keepdims=True)
            aux(b, to_row(step, eye), to_row(count, eye))

    def send_sums(k, s, q, h):
        def aux(b, step, count):
            yaux[k.c, s, h, b, 0:1, :] = step
            yaux[k.c, s, h, b, 1:2, :] = count

        pack(k.c, q, h, lambda zb: ysend.at[k.c, s, h, zb], aux)
        k.sums[s, h] = [
            remote(ysend.at[k.c, s, h], yrecv.at[k.c, s, h], k.at_r(q)),
            remote(yaux.at[k.c, s, h], yauxr.at[k.c, s, h], k.at_r(q)),
        ]

    phase("y_pack")
    order = [(k, 2, k.ro) for k in colours] + [(k, s, q) for k in colours for s, q in ((0, k.rr), (1, k.rl))]
    for k in colours:
        k.sums = {}
    for k, s, q in order:
        accumulate(k.c, *k.rest, q)
        send_sums(k, s, q, 0)
    phase("y_packq")
    for k, s, q in order:
        send_sums(k, s, q, 1)
    phase("y_own")
    for k in colours:
        accumulate(k.c, 2, 6, k.r)

    def unpack(k, s, h):
        for b in range(HROWS // LANES):
            step = to_col(yauxr[k.c, s, h, b, 0:1, :], lane_eye(LANES))
            for j in range(LANES // OWN):
                high, low = decode(yrecv[k.c, s, h, b * (LANES // OWN) + j], step[j * OWN : (j + 1) * OWN])
                base = b * LANES + j * OWN
                acc[k.c, k.r, h, pl.ds(base, PAIRS), :] += high
                acc[k.c, k.r, h, pl.ds(base + PAIRS, PAIRS), :] += low

    zcopies = {}

    def z_send(h):
        phase(f"y_unpack{h}")
        for s in (0, 1, 2):
            for k in colours:
                arrive(k.sums[s, h])
                unpack(k, s, h)
        phase(f"z_pack{h}")
        for k in colours:
            def aux(b, step, count, k=k):
                zaux[h, b, 2 * k.c : 2 * k.c + 1, :] = step
                for s in range(3):
                    count = count + yauxr[k.c, s, h, b, 1:2, :]
                zaux[h, b, 2 * k.c + 1 : 2 * k.c + 2, :] = count

            pack(k.c, k.r, h, lambda zb, k=k: zsend.at[h, zb, k.c], aux)
        for d in (4, 3, 5, 2, 6, 1, 7):
            to = zat(d)
            zcopies[h, d] = [
                remote(zaux.at[h, to // (LANES // OWN)], zauxr.at[h, d - 1], at_z(to)),
                remote(zsend.at[h, to], zrecv.at[h, d - 1], at_z(to)),
            ]

    def own_to_slot(h, k, s, device):
        return [
            remote(ref.at[h, k.c, k.f, 0, z], ref.at[h, k.c, k.f, s, z], device) for ref in (words_ref, steps_ref)
        ]

    def z_sum(h):
        phase(f"z_sum{h}")
        mine = lane_eye(OWN, lax.rem(z, LANES // OWN) * OWN)
        for k in colours:
            sums = acc[k.c, k.r, h, pl.ds(pl.multiple_of(z * OWN, OWN), OWN), :]
            k.high, k.low = sums[:PAIRS], sums[PAIRS:]
            k.count = zaux[h, z // (LANES // OWN), 2 * k.c + 1 : 2 * k.c + 2, :]
        for d in (1, 7, 2, 6, 3, 5, 4):
            arrive(zcopies[h, d])
            for k in colours:
                step = to_col(zauxr[h, d - 1, 2 * k.c : 2 * k.c + 1, :], mine)
                high, low = decode(zrecv[h, d - 1, k.c], step)
                k.high, k.low = k.high + high, k.low + low
                k.count = k.count + zauxr[h, d - 1, 2 * k.c + 1 : 2 * k.c + 2, :]
        phase(f"fresh{h}")
        for k in colours:
            count = to_col(k.count, mine)
            rows = pl.ds(pl.multiple_of(k.r * CROWS + h * HROWS + z * OWN, OWN), OWN)
            prior = cv[0, rows, k.cols(k.f)].astype(jnp.float32)
            sums = jnp.concatenate([k.high, k.low], axis=0)
            code, step = encode(jnp.where(count > 0.5, sums / jnp.maximum(count, 1.0), prior))
            words_ref[h, k.c, k.f, 0, z] = pair(code)
            steps_ref[h, k.c, k.f, 0, z] = to_row(step, lane_eye(OWN))
            to_slots = ((2, k.ro), (3, k.rr), (1, k.rl))
            k.start[h] = sum((own_to_slot(h, k, s, k.at_r(to)) for s, to in to_slots), [])
        for k in colours if h == 0 else ():
            for way in (1, -1):
                to_slots = ((2, k.ro), (3, k.rr), (1, k.rl), (0, k.r))
                k.hops[h, way, 1] = sum((own_to_slot(h, k, s, k.at_rz(to, zat(way))) for s, to in to_slots), [])

    def group(h, k, f, zc, device):
        copies = []
        for ref in (words_ref, steps_ref):
            piece = ref.at[h, k.c, f, :, zc]
            copies.append(remote(piece, piece, device))
        return copies

    def hop(h, k, way, n):
        k.hops[h, way, n] = group(h, k, k.f, zat(-way * (n - 1)), at_z(zat(way)))

    def spread(h, k, d):
        targets = (k.fr, k.fl, k.fo) if (h, d) in STRAIGHT else (k.fr, k.fl)
        k.side[h, d] = [group(h, k, k.f, zat(d), k.at_f(to)) for to in targets]

    def left_first(d):
        return d in (0, 1, 2, 3)

    def across(h, *ds):
        phase(f"g_x{h}")
        for d in ds:
            for k in colours:
                from_left, from_right = k.side[h, d]
                if left_first(d):
                    arrive(from_left)
                    k.last[h, d] = group(h, k, k.fl, zat(d), k.at_f(k.fr)) + from_right
                else:
                    arrive(from_right)
                    k.last[h, d] = group(h, k, k.fr, zat(d), k.at_f(k.fl)) + from_left

    def finish(groups):
        def block(s, carry):
            for h, k, f, d in groups:
                zc = zat(d)
                step = to_col(steps_ref[h, k.c, f, s, zc], lane_eye(OWN))
                high, low = decode(words_ref[h, k.c, f, s, zc], step)
                base = pl.multiple_of(lax.rem(k.r + s, N) * CROWS + h * HROWS + zc * OWN, OWN)
                out_ref[pl.ds(base, PAIRS), k.cols(f)] = high
                out_ref[pl.ds(base + PAIRS, PAIRS), k.cols(f)] = low
            return carry

        lax.fori_loop(0, N, block, 0)

    def own_done(h, *ds):
        return [(h, k, k.f, d) for k in colours for d in ds]

    def first_done(h, *ds):
        return [(h, k, k.fl if left_first(d) else k.fr, d) for k in colours for d in ds]

    def last_done(h, *ds):
        groups = []
        for k in colours:
            for d in ds:
                if (h, d) in STRAIGHT:
                    arrive(sum(k.side[h, d], []))
                    groups += [(h, k, f, d) for f in (k.fl, k.fr, k.fo)]
                else:
                    arrive(k.last[h, d])
                    groups += [(h, k, f, d) for f in (k.fo, k.fr if left_first(d) else k.fl)]
        return groups

    def sides_done(h, *ds):
        for k in colours:
            for d in ds:
                arrive(sum(k.side[h, d], []))
        return [(h, k, f, d) for k in colours for d in ds for f in (k.fl, k.fr)]

    def opposite_hop(h):
        for k in colours:
            k.opposite[h] = sum((group(h, k, k.fo, z, at_z(zat(way))) for way in (1, -1)), [])

    def opposite_done(h):
        for k in colours:
            arrive(k.opposite[h])
        return [(h, k, k.fo, d) for k in colours for d in (-1, 1)]

    def far_way(k):
        return 1 - 2 * k.c

    def gather_rows(h):
        phase(f"g_r{h}")
        for k in colours:
            arrive(k.start[h])
            if h == 1:
                hop(h, k, 1, 1)
                hop(h, k, -1, 1)
            spread(h, k, 0)

    def z_round(h, n):
        phase(f"g_z{n}h{h}")
        for k in colours:
            for way in (1, -1):
                if n < 4 or way == far_way(k):
                    arrive(k.hops[h, way, n])
                    if n < 3 or (n == 3 and way == far_way(k)):
                        hop(h, k, way, n + 1)
            for d in (-n, n) if n < 4 else (4,):
                spread(h, k, d)

    for k in colours:
        k.hops, k.side, k.start, k.last, k.opposite = {}, {}, {}, {}, {}
    z_send(0)
    phase("dist1a")
    c_p.wait_recv()
    distances(1, 0, 4)
    z_send(1)
    phase("dist1b")
    distances(1, 4, 2)
    early = list(used)
    z_sum(0)
    phase("dist1c")
    distances(1, 6, 2)
    eye = lane_eye(LANES)
    for b in range(ROWS // LANES):
        part = pv[pl.ds(b * LANES, LANES), :].astype(jnp.float32)
        square = to_row(jnp.sum(part * part, axis=1, keepdims=True), eye)
        lanes = pl.ds(b * LANES, LANES)
        cost_ref[:, lanes] = (square + jnp.min(best[:, lanes], axis=0, keepdims=True)) * (1.0 / 1024)
    z_sum(1)
    for copy in early:
        copy.wait_send()
    gather_rows(0)
    z_round(0, 1)
    gather_rows(1)
    across(0, 0)
    phase("g_f0")
    finish(own_done(0, 0, -1, 1) + first_done(0, 0))
    z_round(0, 2)
    z_round(1, 1)
    across(1, 0)
    phase("g_f1")
    done = last_done(0, 0)
    opposite_hop(0)
    finish(own_done(0, -2, 2) + own_done(1, 0) + done)
    z_round(0, 3)
    z_round(1, 2)
    across(0, -2, 2)
    phase("g_f2")
    done = last_done(1, 0)
    opposite_hop(1)
    finish(own_done(0, -3, 3) + own_done(1, -1, 1) + first_done(0, -2, 2) + first_done(1, 0) + sides_done(0, -1, 1) + done)
    z_round(0, 4)
    z_round(1, 3)
    across(0, -3, 3)
    across(1, -2, 2)
    phase("g_f3")
    finish(own_done(0, 4) + own_done(1, -2, 2) + opposite_done(0))
    z_round(1, 4)
    across(0, 4)
    across(1, *(d for d in (-3, 3) if (1, d) not in STRAIGHT))
    phase("g_f4")
    finish(own_done(1, -3, 3, 4) + first_done(0, -3, 3) + first_done(1, -2, 2) + last_done(0, -2, 2) + sides_done(1, -1, 1))
    across(1, *(d for d in (4,) if (1, d) not in STRAIGHT))
    phase("g_f5")
    finish(first_done(0, 4) + first_done(1, *(d for d in (-3, 3, 4) if (1, d) not in STRAIGHT)) + last_done(0, -3, 3) + opposite_done(1))
    phase("g_f6")
    finish(last_done(0, 4) + last_done(1, -2, 2))
    phase("g_f7")
    finish(last_done(1, -3, 3))
    phase("g_f8")
    finish(last_done(1, 4))
    phase("w_send")
    for copy in used[len(early) :]:
        copy.wait_send()
    phase(None)
    assert len(used) == N_COPIES, len(used)


N_COPIES = 382
STRAIGHT = ((1, 4),)


def put_kernel(rows_ref, cost_ref, rows_hbm, cost_hbm, sems):
    puts = [pltpu.make_async_copy(cost_ref, cost_hbm, sems.at[N])]
    for q in range(N):
        rows = pl.ds(q * CROWS, CROWS)
        puts.append(pltpu.make_async_copy(rows_ref.at[rows], rows_hbm.at[rows], sems.at[q]))
    for put in puts:
        put.start()
    for put in puts:
        put.wait()


def shards(points, centroids, assign, keep_mask):
    vmem = pl.BlockSpec(memory_space=pltpu.VMEM)
    hbm = pl.BlockSpec(memory_space=pltpu.HBM)
    dma = pltpu.SemaphoreType.DMA
    f32, i32, bf16 = jnp.float32, jnp.int32, jnp.bfloat16
    args = (points, centroids, assign.reshape(1, ROWS), keep_mask.reshape(1, ROWS))
    rows, cost = pl.pallas_call(
        update_kernel,
        out_shape=(
            jax.ShapeDtypeStruct((2048, 1024), f32),
            jax.ShapeDtypeStruct((1, ROWS), f32),
        ),
        in_specs=[hbm] * 4,
        out_specs=(vmem, vmem),
        scratch_shapes=[
            pltpu.VMEM((2, 2, N, N, NZ, PAIRS, LANES), i32),
            pltpu.VMEM((2, 2, N, N, NZ, 1, LANES), f32),
            pltpu.VMEM((ROWS, 1024), bf16),
            pltpu.VMEM((2, 2048, 1024), bf16),
            pltpu.VMEM((2, 1, ROWS), i32),
            pltpu.VMEM((2 * ROWS, 2 * LANES), bf16),
            pltpu.VMEM((2, 6 * ROWS, LANES), bf16),
            pltpu.VMEM((1, 2 * ROWS), i32),
            pltpu.VMEM((2, 1, 6 * ROWS), i32),
            pltpu.VMEM((2, 2, ROWS // 2, LANES), bf16),
            pltpu.VMEM((8, ROWS), f32),
            pltpu.VMEM((2, N, 2, HROWS, LANES), f32),
            pltpu.VMEM((2, N, 2, HROWS, LANES), bf16),
            pltpu.VMEM((2, 3, 2, NZ, PAIRS, LANES), i32),
            pltpu.VMEM((2, 3, 2, 2, 2, LANES), f32),
            pltpu.VMEM((2, 3, 2, NZ, PAIRS, LANES), i32),
            pltpu.VMEM((2, 3, 2, 2, 2, LANES), f32),
            pltpu.VMEM((2, NZ, 2, PAIRS, LANES), i32),
            pltpu.VMEM((2, 2, 4, LANES), f32),
            pltpu.VMEM((2, NZ - 1, 2, PAIRS, LANES), i32),
            pltpu.VMEM((2, NZ - 1, 4, LANES), f32),
            dma((N_COPIES,)), dma((N_COPIES,)), dma((6,)),
        ],
        compiler_params=pltpu.CompilerParams(
            collective_id=0, has_side_effects=True, vmem_limit_bytes=40 * 1024 * 1024
        ),
    )(*(pltpu.with_memory_space_constraint(a, pltpu.HBM) for a in args))
    new_centroids, cost = pl.pallas_call(
        put_kernel,
        out_shape=(jax.ShapeDtypeStruct((2048, 1024), f32), jax.ShapeDtypeStruct((1, ROWS), f32)),
        in_specs=[vmem] * 2,
        out_specs=(hbm, hbm),
        scratch_shapes=[dma((N + 1,))],
        compiler_params=pltpu.CompilerParams(vmem_limit_bytes=1024 * 1024),
        cost_estimate=pl.CostEstimate(flops=0, bytes_accessed=16 << 20, transcendentals=0),
    )(rows, cost)
    return new_centroids, cost.reshape(ROWS)


def solution(mesh):
    grid = Mesh(mesh.devices.reshape(NZ, N, N, 2), ("z", "y", "x", "mp"))
    rows = ("z", "y", "x", "mp")
    in_specs = (P(rows, None), P("mp", None), P(rows), P(rows))
    out_specs = (P("mp", None), P(rows))
    return jax.shard_map(shards, mesh=grid, in_specs=in_specs, out_specs=out_specs, check_vma=False)
```

```python
import jax
import jax.numpy as jnp
from jax import lax
from jax.experimental import pallas as pl
from jax.experimental.pallas import tpu as pltpu
from jax.sharding import Mesh
from jax.sharding import PartitionSpec as P

STEPS = 32000.0
TINY = 2.0**-100
N, NZ = 4, 8
LANES = 128
CROWS = 512
HROWS = CROWS // 2
OWN = HROWS // NZ
PAIRS = OWN // 2
TILE = 256
ROWS = 512
MESH_ID = pl.DeviceIdType.MESH


def encode(v):
    top = jnp.maximum(jnp.max(jnp.abs(v), axis=1, keepdims=True), TINY)
    code = jnp.floor(v * (STEPS / top) + 0.5).astype(jnp.int32)
    return code, top * (1.0 / STEPS)


def pair(code):
    return (code[:PAIRS] << 16) | (code[PAIRS:] & 0xFFFF)


def decode(words, step):
    high = (words >> 16).astype(jnp.float32)
    low = ((words << 16) >> 16).astype(jnp.float32)
    return high * step[:PAIRS], low * step[PAIRS:]


def lane_eye(rows, shift=0):
    at_row = lax.broadcasted_iota(jnp.int32, (rows, LANES), 0)
    at_lane = lax.broadcasted_iota(jnp.int32, (rows, LANES), 1)
    return at_lane == at_row + shift


def to_row(col, eye):
    return jnp.sum(jnp.where(eye, col, 0.0), axis=0, keepdims=True)


def to_col(row, eye):
    return jnp.sum(jnp.where(eye, row, 0.0), axis=1, keepdims=True)


def update_kernel(
    p_hbm, c_hbm, assign_hbm, keep_hbm, out_ref, cost_ref,
    words_ref, steps_ref,
    pv, cv, idv, near0, near, ids0, ids, relay, best, acc, cnt,
    ysend, yaux, yrecv, yauxr, zsend, zaux, zrecv, zauxr,
    send_sem, recv_sem, local_sem,
):
    z, y, x, m = (lax.axis_index(n) for n in ("z", "y", "x", "mp"))
    zat = lambda d: lax.rem(z + d + NZ, NZ)
    used = []
    scopes = []

    def phase(name):
        if scopes:
            scopes.pop().__exit__(None, None, None)
        if name:
            scopes.append(jax.named_scope(name))
            scopes[-1].__enter__()

    def remote(src, dst, device):
        k = len(used)
        copy = pltpu.make_async_remote_copy(
            src_ref=src, dst_ref=dst, send_sem=send_sem.at[k], recv_sem=recv_sem.at[k],
            device_id=device, device_id_type=MESH_ID,
        )
        copy.start()
        used.append(copy)
        return copy

    def arrive(copies):
        for copy in copies:
            copy.wait_recv()

    at_x = lambda to: (z, y, to, m)
    at_y = lambda to: (z, to, x, m)
    at_z = lambda to: (to, y, x, m)
    partner = (z, y, x, 1 - m)

    class Colour:
        def __init__(self, c, first, second, at_first, at_second, at_second_z):
            self.c, self.f, self.r = c, first, second
            self.fr, self.fl, self.fo = (lax.rem(first + d, N) for d in (1, 3, 2))
            self.rr, self.rl, self.ro = (lax.rem(second + d, N) for d in (1, 3, 2))
            self.at_f, self.at_r, self.at_rz = at_first, at_second, at_second_z

        def cols(self, f):
            return pl.ds(pl.multiple_of(self.c * 512 + f * LANES, LANES), LANES)

    at_xz = lambda to, to_z: (to_z, y, to, m)
    at_yz = lambda to, to_z: (to_z, to, x, m)
    colours = (Colour(0, x, y, at_x, at_y, at_yz), Colour(1, y, x, at_y, at_x, at_xz))

    phase("enter")
    loads = [
        pltpu.make_async_copy(p_hbm, pv, local_sem.at[0]),
        pltpu.make_async_copy(assign_hbm, idv.at[0], local_sem.at[1]),
        pltpu.make_async_copy(keep_hbm, idv.at[1], local_sem.at[2]),
    ]
    load_c = pltpu.make_async_copy(c_hbm, cv.at[0], local_sem.at[3])
    for copy in loads + [load_c]:
        copy.start()

    peers = [partner] + [at_z(zat(d)) for d in range(1, NZ)]
    for k in colours:
        peers += [k.at_f(k.fr), k.at_f(k.fl), k.at_f(k.fo)]
        peers += [k.at_rz(to, zat(d)) for to in (k.rr, k.rl, k.ro) for d in (1, -1)]
    barrier = pltpu.get_barrier_semaphore()
    for peer in peers:
        pl.semaphore_signal(barrier, inc=1, device_id=peer, device_id_type=MESH_ID)
    for copy in loads:
        copy.wait()
    ids0[:, :ROWS] = jnp.where(idv[1] > 0, idv[0], -1)
    best[...] = jnp.full(best.shape, jnp.inf, jnp.float32)
    pl.semaphore_wait(barrier, len(peers))

    phase("send_p")

    def slot(s):
        return pl.ds((s - 2) * ROWS, ROWS)

    lo, hi = pl.ds(0, ROWS // 2), pl.ds(ROWS // 2, ROWS // 2)
    mine_ids = ids0.at[:, pl.ds(0, ROWS)]
    for k in colours:
        k.relay_l = remote(pv.at[lo, k.cols(k.fo)], relay.at[k.c, 0], k.at_f(k.fr))
        k.relay_r = remote(pv.at[hi, k.cols(k.fo)], relay.at[k.c, 1], k.at_f(k.fl))
    own = []
    from_p = [remote(mine_ids, ids0.at[:, pl.ds(ROWS, ROWS)], partner)]
    for k in colours:
        lanes = pl.ds(k.c * LANES, LANES)
        own.append(
            pltpu.make_async_copy(pv.at[:, k.cols(k.f)], near0.at[pl.ds(0, ROWS), lanes], local_sem.at[4 + k.c])
        )
        own[-1].start()
        from_p.append(remote(pv.at[:, k.cols(k.f)], near0.at[pl.ds(ROWS, ROWS), lanes], partner))
    for k in colours:
        k.from_l = [
            remote(mine_ids, ids.at[k.c, :, slot(2)], k.at_f(k.fr)),
            remote(pv.at[:, k.cols(k.fr)], near.at[k.c, slot(2)], k.at_f(k.fr)),
        ]
        k.from_r = [
            remote(mine_ids, ids.at[k.c, :, slot(3)], k.at_f(k.fl)),
            remote(pv.at[:, k.cols(k.fl)], near.at[k.c, slot(3)], k.at_f(k.fl)),
        ]
        k.from_o = [remote(mine_ids, ids.at[k.c, :, slot(6)], k.at_f(k.fo))]
    c_p = remote(c_hbm, cv.at[1], partner)

    def distances(s, first, count):
        def tile(t, carry):
            part = cv[s, pl.ds(pl.multiple_of(t * TILE, TILE), TILE), :]
            inner = lax.dot_general(
                part, pv[...], (((1,), (1,)), ((), ())), preferred_element_type=jnp.float32
            )
            wide = part.astype(jnp.float32)
            square = jnp.sum(wide * wide, axis=1, keepdims=True)
            dist = square - 2.0 * inner
            low = jnp.min(dist.reshape(TILE // 8, 8, ROWS), axis=0)
            best[...] = jnp.minimum(best[...], low)
            return carry

        lax.fori_loop(first, first + count, tile, 0)

    def hits(id_row, base):
        local = id_row - base
        local = jnp.where((local >= 0) & (local < TILE), local, -1).astype(jnp.float32)
        width = id_row.shape[1]
        local = jnp.broadcast_to(local, (16, width)).astype(jnp.bfloat16)
        at = lax.broadcasted_iota(jnp.int32, (TILE, LANES), 0).astype(jnp.float32).astype(jnp.bfloat16)
        at = at.reshape(TILE // 16, 16, LANES)
        one, zero = jnp.ones((), jnp.bfloat16), jnp.zeros((), jnp.bfloat16)
        parts = [
            jnp.where(at == local[None, :, i * LANES : (i + 1) * LANES], one, zero).reshape(TILE, LANES)
            for i in range(width // LANES)
        ]
        count = parts[0]
        for part in parts[1:]:
            count = count + part
        return jnp.concatenate(parts, axis=1), count

    def hits_chunk(id_row, base):
        low, count_low = hits(id_row, base)
        high, count_high = hits(id_row, base + TILE)
        return jnp.concatenate([low, high], axis=0), jnp.concatenate([count_low, count_high], axis=0)

    def accumulate(c, first, count, q):
        where = pl.ds((first - 2) * ROWS, count * ROWS)
        hit, number = hits_chunk(ids[c, :, where], m * 2048 + q * CROWS)
        part = jnp.dot(hit, near[c, where, :], preferred_element_type=jnp.float32)
        acc[c, q] += part.reshape(2, HROWS, LANES)
        cnt[c, q] += number.reshape(2, HROWS, LANES)

    def accumulate_others(k, first, count):
        def body(j, carry):
            accumulate(k.c, first, count, lax.rem(k.r + 1 + j, N))
            return carry

        lax.fori_loop(0, N - 1, body, 0)

    def accumulate_own():
        def body(q, carry):
            hit, count = hits_chunk(ids0[...], m * 2048 + q * CROWS)
            part = jnp.dot(hit, near0[...], preferred_element_type=jnp.float32)
            for c in range(2):
                acc[c, q] = part[:, c * LANES : (c + 1) * LANES].reshape(2, HROWS, LANES)
                cnt[c, q] = count.reshape(2, HROWS, LANES)
            return carry

        lax.fori_loop(0, N, body, 0)

    phase("dist0a")
    load_c.wait()
    distances(0, 0, 4)
    phase("w_own")
    for copy in own:
        copy.wait()
    arrive(from_p)
    phase("acc0")
    accumulate_own()
    phase("w_relay")
    for k in colours:
        k.relay_l.wait_recv()
        k.from_o.append(remote(relay.at[k.c, 0], near.at[k.c, pl.ds(4 * ROWS, ROWS // 2)], k.at_f(k.fr)))
        k.relay_r.wait_recv()
        k.from_o.append(remote(relay.at[k.c, 1], near.at[k.c, pl.ds(4 * ROWS + ROWS // 2, ROWS // 2)], k.at_f(k.fl)))
    phase("dist0b")
    distances(0, 4, 4)

    def to_partner(k, source, target):
        return [
            remote(near.at[k.c, slot(source)], near.at[k.c, slot(target)], partner),
            remote(ids.at[k.c, :, slot(source)], ids.at[k.c, :, slot(target)], partner),
        ]

    phase("w_lr")
    for k in colours:
        arrive(k.from_l)
        k.two = to_partner(k, 2, 4)
        arrive(k.from_r)
        k.two += to_partner(k, 3, 5)
    phase("acc1")
    accumulate_others(colours[0], 2, 2)
    phase("w_o")
    for k in colours:
        arrive(k.from_o)
        k.three = to_partner(k, 6, 7)
    phase("acc2")
    accumulate_others(colours[1], 2, 2)
    phase("w_plr")
    for k in colours:
        arrive(k.two)
    phase("w_po")
    for k in colours:
        arrive(k.three)

    def pack(c, q, h, words, aux):
        for b in range(HROWS // LANES):
            eye = lane_eye(LANES)
            rows = pl.ds(b * LANES, LANES)
            code, step = encode(acc[c, q, h, rows, :])
            for j in range(LANES // OWN):
                words(b * (LANES // OWN) + j)[...] = pair(code[j * OWN : (j + 1) * OWN])
            count = jnp.sum(cnt[c, q, h, rows, :].astype(jnp.float32), axis=1, keepdims=True)
            aux(b, to_row(step, eye), to_row(count, eye))

    def send_sums(k, s, q, h):
        def aux(b, step, count):
            yaux[k.c, s, h, b, 0:1, :] = step
            yaux[k.c, s, h, b, 1:2, :] = count

        pack(k.c, q, h, lambda zb: ysend.at[k.c, s, h, zb], aux)
        k.sums[s, h] = [
            remote(ysend.at[k.c, s, h], yrecv.at[k.c, s, h], k.at_r(q)),
            remote(yaux.at[k.c, s, h], yauxr.at[k.c, s, h], k.at_r(q)),
        ]

    phase("y_pack")
    order = [(k, 2, k.ro) for k in colours] + [(k, s, q) for k in colours for s, q in ((0, k.rr), (1, k.rl))]
    for k in colours:
        k.sums = {}
    for k, s, q in order:
        accumulate(k.c, 4, 4, q)
        send_sums(k, s, q, 0)
    phase("y_packq")
    for k, s, q in order:
        send_sums(k, s, q, 1)
    phase("y_own")
    for k in colours:
        accumulate(k.c, 2, 6, k.r)

    def unpack(k, s, h):
        for b in range(HROWS // LANES):
            step = to_col(yauxr[k.c, s, h, b, 0:1, :], lane_eye(LANES))
            for j in range(LANES // OWN):
                high, low = decode(yrecv[k.c, s, h, b * (LANES // OWN) + j], step[j * OWN : (j + 1) * OWN])
                base = b * LANES + j * OWN
                acc[k.c, k.r, h, pl.ds(base, PAIRS), :] += high
                acc[k.c, k.r, h, pl.ds(base + PAIRS, PAIRS), :] += low

    zcopies = {}

    def z_send(h):
        phase(f"y_unpack{h}")
        for s in (0, 1, 2):
            for k in colours:
                arrive(k.sums[s, h])
                unpack(k, s, h)
        phase(f"z_pack{h}")
        for k in colours:
            def aux(b, step, count, k=k):
                zaux[h, b, 2 * k.c : 2 * k.c + 1, :] = step
                for s in range(3):
                    count = count + yauxr[k.c, s, h, b, 1:2, :]
                zaux[h, b, 2 * k.c + 1 : 2 * k.c + 2, :] = count

            pack(k.c, k.r, h, lambda zb, k=k: zsend.at[h, zb, k.c], aux)
        for d in (4, 3, 5, 2, 6, 1, 7):
            to = zat(d)
            zcopies[h, d] = [
                remote(zaux.at[h, to // (LANES // OWN)], zauxr.at[h, d - 1], at_z(to)),
                remote(zsend.at[h, to], zrecv.at[h, d - 1], at_z(to)),
            ]

    def own_to_slot(h, k, s, device):
        return [
            remote(ref.at[h, k.c, k.f, 0, z], ref.at[h, k.c, k.f, s, z], device) for ref in (words_ref, steps_ref)
        ]

    def z_sum(h):
        phase(f"z_sum{h}")
        mine = lane_eye(OWN, lax.rem(z, LANES // OWN) * OWN)
        for k in colours:
            sums = acc[k.c, k.r, h, pl.ds(pl.multiple_of(z * OWN, OWN), OWN), :]
            k.high, k.low = sums[:PAIRS], sums[PAIRS:]
            k.count = zaux[h, z // (LANES // OWN), 2 * k.c + 1 : 2 * k.c + 2, :]
        for d in (1, 7, 2, 6, 3, 5, 4):
            arrive(zcopies[h, d])
            for k in colours:
                step = to_col(zauxr[h, d - 1, 2 * k.c : 2 * k.c + 1, :], mine)
                high, low = decode(zrecv[h, d - 1, k.c], step)
                k.high, k.low = k.high + high, k.low + low
                k.count = k.count + zauxr[h, d - 1, 2 * k.c + 1 : 2 * k.c + 2, :]
        phase(f"fresh{h}")
        for k in colours:
            count = to_col(k.count, mine)
            rows = pl.ds(pl.multiple_of(k.r * CROWS + h * HROWS + z * OWN, OWN), OWN)
            prior = cv[0, rows, k.cols(k.f)].astype(jnp.float32)
            sums = jnp.concatenate([k.high, k.low], axis=0)
            code, step = encode(jnp.where(count > 0.5, sums / jnp.maximum(count, 1.0), prior))
            words_ref[h, k.c, k.f, 0, z] = pair(code)
            steps_ref[h, k.c, k.f, 0, z] = to_row(step, lane_eye(OWN))
            to_slots = ((2, k.ro), (3, k.rr), (1, k.rl))
            k.start[h] = sum((own_to_slot(h, k, s, k.at_r(to)) for s, to in to_slots), [])
        for k in colours if h == 0 else ():
            for way in (1, -1):
                to_slots = ((2, k.ro), (3, k.rr), (1, k.rl), (0, k.r))
                k.hops[h, way, 1] = sum((own_to_slot(h, k, s, k.at_rz(to, zat(way))) for s, to in to_slots), [])

    def group(h, k, f, zc, device):
        copies = []
        for ref in (words_ref, steps_ref):
            piece = ref.at[h, k.c, f, :, zc]
            copies.append(remote(piece, piece, device))
        return copies

    def hop(h, k, way, n):
        k.hops[h, way, n] = group(h, k, k.f, zat(-way * (n - 1)), at_z(zat(way)))

    def spread(h, k, d):
        targets = (k.fr, k.fl, k.fo) if (h, d) in STRAIGHT else (k.fr, k.fl)
        k.side[h, d] = [group(h, k, k.f, zat(d), k.at_f(to)) for to in targets]

    def relayed(h, ds):
        return [d for d in ds if (h, d) not in STRAIGHT]

    def left_first(d):
        return d in (0, 1, 2, 3)

    def across(h, *ds):
        phase(f"g_x{h}")
        for d in relayed(h, ds):
            for k in colours:
                from_left, from_right = k.side[h, d]
                if left_first(d):
                    arrive(from_left)
                    k.last[h, d] = group(h, k, k.fl, zat(d), k.at_f(k.fr)) + from_right
                else:
                    arrive(from_right)
                    k.last[h, d] = group(h, k, k.fr, zat(d), k.at_f(k.fl)) + from_left

    def finish(groups):
        def block(s, carry):
            for h, k, f, d in groups:
                zc = zat(d)
                step = to_col(steps_ref[h, k.c, f, s, zc], lane_eye(OWN))
                high, low = decode(words_ref[h, k.c, f, s, zc], step)
                base = pl.multiple_of(lax.rem(k.r + s, N) * CROWS + h * HROWS + zc * OWN, OWN)
                out_ref[pl.ds(base, PAIRS), k.cols(f)] = high
                out_ref[pl.ds(base + PAIRS, PAIRS), k.cols(f)] = low
            return carry

        lax.fori_loop(0, N, block, 0)

    def own_done(h, *ds):
        return [(h, k, k.f, d) for k in colours for d in ds]

    def first_done(h, *ds):
        return [(h, k, k.fl if left_first(d) else k.fr, d) for k in colours for d in relayed(h, ds)]

    def last_done(h, *ds):
        groups = []
        for k in colours:
            for d in ds:
                if (h, d) in STRAIGHT:
                    arrive(sum(k.side[h, d], []))
                    groups += [(h, k, f, d) for f in (k.fl, k.fr, k.fo)]
                else:
                    arrive(k.last[h, d])
                    groups += [(h, k, f, d) for f in (k.fo, k.fr if left_first(d) else k.fl)]
        return groups

    def sides_done(h, *ds):
        for k in colours:
            for d in ds:
                arrive(sum(k.side[h, d], []))
        return [(h, k, f, d) for k in colours for d in ds for f in (k.fl, k.fr)]

    def opposite_hop(h):
        for k in colours:
            k.opposite[h] = sum((group(h, k, k.fo, z, at_z(zat(way))) for way in (1, -1)), [])

    def opposite_done(h):
        for k in colours:
            arrive(k.opposite[h])
        return [(h, k, k.fo, d) for k in colours for d in (-1, 1)]

    def far_way(k):
        return 1 - 2 * k.c

    def gather_rows(h):
        phase(f"g_r{h}")
        for k in colours:
            arrive(k.start[h])
            if h == 1:
                hop(h, k, 1, 1)
                hop(h, k, -1, 1)
            spread(h, k, 0)

    def z_round(h, n):
        phase(f"g_z{n}h{h}")
        for k in colours:
            for way in (1, -1):
                if n < 4 or way == far_way(k):
                    arrive(k.hops[h, way, n])
                    if n < 3 or (n == 3 and way == far_way(k)):
                        hop(h, k, way, n + 1)
            for d in (-n, n) if n < 4 else (4,):
                spread(h, k, d)

    for k in colours:
        k.hops, k.side, k.start, k.last, k.opposite = {}, {}, {}, {}, {}
    z_send(0)
    phase("dist1a")
    c_p.wait_recv()
    distances(1, 0, 4)
    z_send(1)
    phase("dist1b")
    distances(1, 4, 2)
    early = list(used)
    z_sum(0)
    phase("dist1c")
    distances(1, 6, 2)
    eye = lane_eye(LANES)
    for b in range(ROWS // LANES):
        part = pv[pl.ds(b * LANES, LANES), :].astype(jnp.float32)
        square = to_row(jnp.sum(part * part, axis=1, keepdims=True), eye)
        lanes = pl.ds(b * LANES, LANES)
        cost_ref[:, lanes] = (square + jnp.min(best[:, lanes], axis=0, keepdims=True)) * (1.0 / 1024)
    z_sum(1)
    for copy in early:
        copy.wait_send()
    gather_rows(0)
    z_round(0, 1)
    gather_rows(1)
    across(0, 0)
    phase("g_f0")
    finish(own_done(0, 0, -1, 1) + first_done(0, 0))
    z_round(0, 2)
    z_round(1, 1)
    across(1, 0)
    phase("g_f1")
    done = last_done(0, 0)
    opposite_hop(0)
    finish(own_done(0, -2, 2) + own_done(1, 0) + done)
    z_round(0, 3)
    z_round(1, 2)
    across(0, -2, 2)
    phase("g_f2")
    done = last_done(1, 0)
    opposite_hop(1)
    finish(own_done(0, -3, 3) + own_done(1, -1, 1) + first_done(0, -2, 2) + first_done(1, 0) + sides_done(0, -1, 1) + done)
    z_round(0, 4)
    z_round(1, 3)
    across(0, -3, 3)
    across(1, -2, 2)
    phase("g_f3")
    finish(own_done(0, 4) + own_done(1, -2, 2) + opposite_done(0))
    z_round(1, 4)
    across(0, 4)
    across(1, -3, 3)
    phase("g_f4")
    finish(own_done(1, -3, 3, 4) + first_done(0, -3, 3) + first_done(1, -2, 2) + last_done(0, -2, 2) + sides_done(1, -1, 1))
    across(1, 4)
    phase("g_f5")
    finish(first_done(0, 4) + first_done(1, -3, 3, 4) + last_done(0, -3, 3) + opposite_done(1))
    phase("g_f6")
    finish(last_done(0, 4) + last_done(1, -2, 2))
    phase("g_f7")
    finish(last_done(1, -3, 3))
    for copy in used[len(early) : -24]:
        copy.wait_send()
    phase("g_f8")
    finish(last_done(1, 4))
    phase("w_send")
    for copy in used[-24:]:
        copy.wait_send()
    phase(None)
    assert len(used) == N_COPIES, len(used)


N_COPIES = 382
STRAIGHT = ((1, 4), (1, 3), (1, -3), (0, 4))


def put_kernel(rows_ref, cost_ref, rows_hbm, cost_hbm, sems):
    puts = [pltpu.make_async_copy(cost_ref, cost_hbm, sems.at[N])]
    for q in range(N):
        rows = pl.ds(q * CROWS, CROWS)
        puts.append(pltpu.make_async_copy(rows_ref.at[rows], rows_hbm.at[rows], sems.at[q]))
    for put in puts:
        put.start()
    for put in puts:
        put.wait()


def shards(points, centroids, assign, keep_mask):
    vmem = pl.BlockSpec(memory_space=pltpu.VMEM)
    hbm = pl.BlockSpec(memory_space=pltpu.HBM)
    dma = pltpu.SemaphoreType.DMA
    f32, i32, bf16 = jnp.float32, jnp.int32, jnp.bfloat16
    args = (points, centroids, assign.reshape(1, ROWS), keep_mask.reshape(1, ROWS))
    rows, cost = pl.pallas_call(
        update_kernel,
        out_shape=(
            jax.ShapeDtypeStruct((2048, 1024), f32),
            jax.ShapeDtypeStruct((1, ROWS), f32),
        ),
        in_specs=[hbm] * 4,
        out_specs=(vmem, vmem),
        scratch_shapes=[
            pltpu.VMEM((2, 2, N, N, NZ, PAIRS, LANES), i32),
            pltpu.VMEM((2, 2, N, N, NZ, 1, LANES), f32),
            pltpu.VMEM((ROWS, 1024), bf16),
            pltpu.VMEM((2, 2048, 1024), bf16),
            pltpu.VMEM((2, 1, ROWS), i32),
            pltpu.VMEM((2 * ROWS, 2 * LANES), bf16),
            pltpu.VMEM((2, 6 * ROWS, LANES), bf16),
            pltpu.VMEM((1, 2 * ROWS), i32),
            pltpu.VMEM((2, 1, 6 * ROWS), i32),
            pltpu.VMEM((2, 2, ROWS // 2, LANES), bf16),
            pltpu.VMEM((8, ROWS), f32),
            pltpu.VMEM((2, N, 2, HROWS, LANES), f32),
            pltpu.VMEM((2, N, 2, HROWS, LANES), bf16),
            pltpu.VMEM((2, 3, 2, NZ, PAIRS, LANES), i32),
            pltpu.VMEM((2, 3, 2, 2, 2, LANES), f32),
            pltpu.VMEM((2, 3, 2, NZ, PAIRS, LANES), i32),
            pltpu.VMEM((2, 3, 2, 2, 2, LANES), f32),
            pltpu.VMEM((2, NZ, 2, PAIRS, LANES), i32),
            pltpu.VMEM((2, 2, 4, LANES), f32),
            pltpu.VMEM((2, NZ - 1, 2, PAIRS, LANES), i32),
            pltpu.VMEM((2, NZ - 1, 4, LANES), f32),
            dma((N_COPIES,)), dma((N_COPIES,)), dma((6,)),
        ],
        compiler_params=pltpu.CompilerParams(
            collective_id=0, has_side_effects=True, vmem_limit_bytes=40 * 1024 * 1024
        ),
    )(*(pltpu.with_memory_space_constraint(a, pltpu.HBM) for a in args))
    new_centroids, cost = pl.pallas_call(
        put_kernel,
        out_shape=(jax.ShapeDtypeStruct((2048, 1024), f32), jax.ShapeDtypeStruct((1, ROWS), f32)),
        in_specs=[vmem] * 2,
        out_specs=(hbm, hbm),
        scratch_shapes=[dma((N + 1,))],
        compiler_params=pltpu.CompilerParams(vmem_limit_bytes=1024 * 1024),
        cost_estimate=pl.CostEstimate(flops=0, bytes_accessed=16 << 20, transcendentals=0),
    )(rows, cost)
    return new_centroids, cost.reshape(ROWS)


def solution(mesh):
    grid = Mesh(mesh.devices.reshape(NZ, N, N, 2), ("z", "y", "x", "mp"))
    rows = ("z", "y", "x", "mp")
    in_specs = (P(rows, None), P("mp", None), P(rows), P(rows))
    out_specs = (P("mp", None), P(rows))
    return jax.shard_map(shards, mesh=grid, in_specs=in_specs, out_specs=out_specs, check_vma=False)
```

```python
import jax
import jax.numpy as jnp
from jax import lax
from jax.experimental import pallas as pl
from jax.experimental.pallas import tpu as pltpu
from jax.sharding import Mesh
from jax.sharding import PartitionSpec as P

STEPS = 32000.0
TINY = 2.0**-100
N, NZ = 4, 8
LANES = 128
CROWS = 512
HROWS = CROWS // 2
OWN = HROWS // NZ
PAIRS = OWN // 2
TILE = 256
ROWS = 512
MESH_ID = pl.DeviceIdType.MESH


def encode(v):
    top = jnp.maximum(jnp.max(jnp.abs(v), axis=1, keepdims=True), TINY)
    code = jnp.floor(v * (STEPS / top) + 0.5).astype(jnp.int32)
    return code, top * (1.0 / STEPS)


def pair(code):
    return (code[:PAIRS] << 16) | (code[PAIRS:] & 0xFFFF)


def decode(words, step):
    high = (words >> 16).astype(jnp.float32)
    low = ((words << 16) >> 16).astype(jnp.float32)
    return high * step[:PAIRS], low * step[PAIRS:]


def lane_eye(rows, shift=0):
    at_row = lax.broadcasted_iota(jnp.int32, (rows, LANES), 0)
    at_lane = lax.broadcasted_iota(jnp.int32, (rows, LANES), 1)
    return at_lane == at_row + shift


def to_row(col, eye):
    return jnp.sum(jnp.where(eye, col, 0.0), axis=0, keepdims=True)


def to_col(row, eye):
    return jnp.sum(jnp.where(eye, row, 0.0), axis=1, keepdims=True)


def update_kernel(
    p_hbm, c_hbm, assign_hbm, keep_hbm, out_ref, cost_ref,
    words_ref, steps_ref,
    pv, cv, idv, near0, near, ids0, ids, relay, best, acc, cnt,
    ysend, yaux, yrecv, yauxr, zsend, zaux, zrecv, zauxr,
    send_sem, recv_sem, local_sem,
):
    z, y, x, m = (lax.axis_index(n) for n in ("z", "y", "x", "mp"))
    zat = lambda d: lax.rem(z + d + NZ, NZ)
    used = []
    scopes = []

    def phase(name):
        if scopes:
            scopes.pop().__exit__(None, None, None)
        if name:
            scopes.append(jax.named_scope(name))
            scopes[-1].__enter__()

    def remote(src, dst, device):
        k = len(used)
        copy = pltpu.make_async_remote_copy(
            src_ref=src, dst_ref=dst, send_sem=send_sem.at[k], recv_sem=recv_sem.at[k],
            device_id=device, device_id_type=MESH_ID,
        )
        copy.start()
        used.append(copy)
        return copy

    def arrive(copies):
        for copy in copies:
            copy.wait_recv()

    at_x = lambda to: (z, y, to, m)
    at_y = lambda to: (z, to, x, m)
    at_z = lambda to: (to, y, x, m)
    partner = (z, y, x, 1 - m)

    class Colour:
        def __init__(self, c, first, second, at_first, at_second, at_second_z):
            self.c, self.f, self.r = c, first, second
            self.fr, self.fl, self.fo = (lax.rem(first + d, N) for d in (1, 3, 2))
            self.rr, self.rl, self.ro = (lax.rem(second + d, N) for d in (1, 3, 2))
            self.at_f, self.at_r, self.at_rz = at_first, at_second, at_second_z

        def cols(self, f):
            return pl.ds(pl.multiple_of(self.c * 512 + f * LANES, LANES), LANES)

    at_xz = lambda to, to_z: (to_z, y, to, m)
    at_yz = lambda to, to_z: (to_z, to, x, m)
    colours = (Colour(0, x, y, at_x, at_y, at_yz), Colour(1, y, x, at_y, at_x, at_xz))

    phase("enter")
    loads = [
        pltpu.make_async_copy(p_hbm, pv, local_sem.at[0]),
        pltpu.make_async_copy(assign_hbm, idv.at[0], local_sem.at[1]),
        pltpu.make_async_copy(keep_hbm, idv.at[1], local_sem.at[2]),
    ]
    load_c = pltpu.make_async_copy(c_hbm, cv.at[0], local_sem.at[3])
    for copy in loads + [load_c]:
        copy.start()

    peers = [partner] + [at_z(zat(d)) for d in range(1, NZ)]
    for k in colours:
        peers += [k.at_f(k.fr), k.at_f(k.fl), k.at_f(k.fo)]
        peers += [k.at_rz(to, zat(d)) for to in (k.rr, k.rl, k.ro) for d in (1, -1)]
    barrier = pltpu.get_barrier_semaphore()
    for peer in peers:
        pl.semaphore_signal(barrier, inc=1, device_id=peer, device_id_type=MESH_ID)
    for copy in loads:
        copy.wait()
    ids0[:, :ROWS] = jnp.where(idv[1] > 0, idv[0], -1)
    best[...] = jnp.full(best.shape, jnp.inf, jnp.float32)
    pl.semaphore_wait(barrier, len(peers))

    phase("send_p")

    def slot(s):
        return pl.ds((s - 2) * ROWS, ROWS)

    lo, hi = pl.ds(0, ROWS // 2), pl.ds(ROWS // 2, ROWS // 2)
    mine_ids = ids0.at[:, pl.ds(0, ROWS)]
    for k in colours:
        k.relay_l = remote(pv.at[lo, k.cols(k.fo)], relay.at[k.c, 0], k.at_f(k.fr))
        k.relay_r = remote(pv.at[hi, k.cols(k.fo)], relay.at[k.c, 1], k.at_f(k.fl))
    own = []
    from_p = [remote(mine_ids, ids0.at[:, pl.ds(ROWS, ROWS)], partner)]
    for k in colours:
        lanes = pl.ds(k.c * LANES, LANES)
        own.append(
            pltpu.make_async_copy(pv.at[:, k.cols(k.f)], near0.at[pl.ds(0, ROWS), lanes], local_sem.at[4 + k.c])
        )
        own[-1].start()
        from_p.append(remote(pv.at[:, k.cols(k.f)], near0.at[pl.ds(ROWS, ROWS), lanes], partner))
    for k in colours:
        k.from_l = [
            remote(mine_ids, ids.at[k.c, :, slot(2)], k.at_f(k.fr)),
            remote(pv.at[:, k.cols(k.fr)], near.at[k.c, slot(2)], k.at_f(k.fr)),
        ]
        k.from_r = [
            remote(mine_ids, ids.at[k.c, :, slot(3)], k.at_f(k.fl)),
            remote(pv.at[:, k.cols(k.fl)], near.at[k.c, slot(3)], k.at_f(k.fl)),
        ]
        k.from_o = [remote(mine_ids, ids.at[k.c, :, slot(6)], k.at_f(k.fo))]
    c_p = remote(c_hbm, cv.at[1], partner)

    def distances(s, first, count):
        def tile(t, carry):
            part = cv[s, pl.ds(pl.multiple_of(t * TILE, TILE), TILE), :]
            inner = lax.dot_general(
                part, pv[...], (((1,), (1,)), ((), ())), preferred_element_type=jnp.float32
            )
            wide = part.astype(jnp.float32)
            square = jnp.sum(wide * wide, axis=1, keepdims=True)
            dist = square - 2.0 * inner
            low = jnp.min(dist.reshape(TILE // 8, 8, ROWS), axis=0)
            best[...] = jnp.minimum(best[...], low)
            return carry

        lax.fori_loop(first, first + count, tile, 0)

    def hits(id_row, base):
        local = id_row - base
        local = jnp.where((local >= 0) & (local < TILE), local, -1).astype(jnp.float32)
        width = id_row.shape[1]
        local = jnp.broadcast_to(local, (16, width)).astype(jnp.bfloat16)
        at = lax.broadcasted_iota(jnp.int32, (TILE, LANES), 0).astype(jnp.float32).astype(jnp.bfloat16)
        at = at.reshape(TILE // 16, 16, LANES)
        one, zero = jnp.ones((), jnp.bfloat16), jnp.zeros((), jnp.bfloat16)
        parts = [
            jnp.where(at == local[None, :, i * LANES : (i + 1) * LANES], one, zero).reshape(TILE, LANES)
            for i in range(width // LANES)
        ]
        count = parts[0]
        for part in parts[1:]:
            count = count + part
        return jnp.concatenate(parts, axis=1), count

    def hits_chunk(id_row, base):
        low, count_low = hits(id_row, base)
        high, count_high = hits(id_row, base + TILE)
        return jnp.concatenate([low, high], axis=0), jnp.concatenate([count_low, count_high], axis=0)

    def accumulate(c, first, count, q):
        where = pl.ds((first - 2) * ROWS, count * ROWS)
        hit, number = hits_chunk(ids[c, :, where], m * 2048 + q * CROWS)
        part = jnp.dot(hit, near[c, where, :], preferred_element_type=jnp.float32)
        acc[c, q] += part.reshape(2, HROWS, LANES)
        cnt[c, q] += number.reshape(2, HROWS, LANES)

    def accumulate_others(k, first, count):
        def body(j, carry):
            accumulate(k.c, first, count, lax.rem(k.r + 1 + j, N))
            return carry

        lax.fori_loop(0, N - 1, body, 0)

    def accumulate_own():
        def body(q, carry):
            hit, count = hits_chunk(ids0[...], m * 2048 + q * CROWS)
            part = jnp.dot(hit, near0[...], preferred_element_type=jnp.float32)
            for c in range(2):
                acc[c, q] = part[:, c * LANES : (c + 1) * LANES].reshape(2, HROWS, LANES)
                cnt[c, q] = count.reshape(2, HROWS, LANES)
            return carry

        lax.fori_loop(0, N, body, 0)

    phase("dist0a")
    load_c.wait()
    distances(0, 0, 4)
    phase("w_own")
    for copy in own:
        copy.wait()
    arrive(from_p)
    phase("acc0")
    accumulate_own()
    phase("w_relay")
    for k in colours:
        k.relay_l.wait_recv()
        k.from_o.append(remote(relay.at[k.c, 0], near.at[k.c, pl.ds(4 * ROWS, ROWS // 2)], k.at_f(k.fr)))
        k.relay_r.wait_recv()
        k.from_o.append(remote(relay.at[k.c, 1], near.at[k.c, pl.ds(4 * ROWS + ROWS // 2, ROWS // 2)], k.at_f(k.fl)))
    phase("dist0b")
    distances(0, 4, 4)

    def to_partner(k, source, target):
        return [
            remote(near.at[k.c, slot(source)], near.at[k.c, slot(target)], partner),
            remote(ids.at[k.c, :, slot(source)], ids.at[k.c, :, slot(target)], partner),
        ]

    phase("w_lr")
    for k in colours:
        arrive(k.from_l)
        k.two = to_partner(k, 2, 4)
        arrive(k.from_r)
        k.two += to_partner(k, 3, 5)
    phase("acc1")
    accumulate_others(colours[0], 2, 2)
    phase("w_o")
    for k in colours:
        arrive(k.from_o)
        k.three = to_partner(k, 6, 7)
    phase("acc2")
    accumulate_others(colours[1], 2, 2)
    phase("w_plr")
    for k in colours:
        arrive(k.two)
    phase("w_po")
    for k in colours:
        arrive(k.three)

    def pack(c, q, h, words, aux):
        for b in range(HROWS // LANES):
            eye = lane_eye(LANES)
            rows = pl.ds(b * LANES, LANES)
            code, step = encode(acc[c, q, h, rows, :])
            for j in range(LANES // OWN):
                words(b * (LANES // OWN) + j)[...] = pair(code[j * OWN : (j + 1) * OWN])
            count = jnp.sum(cnt[c, q, h, rows, :].astype(jnp.float32), axis=1, keepdims=True)
            aux(b, to_row(step, eye), to_row(count, eye))

    def send_sums(k, s, q, h):
        def aux(b, step, count):
            yaux[k.c, s, h, b, 0:1, :] = step
            yaux[k.c, s, h, b, 1:2, :] = count

        pack(k.c, q, h, lambda zb: ysend.at[k.c, s, h, zb], aux)
        k.sums[s, h] = [
            remote(ysend.at[k.c, s, h], yrecv.at[k.c, s, h], k.at_r(q)),
            remote(yaux.at[k.c, s, h], yauxr.at[k.c, s, h], k.at_r(q)),
        ]

    phase("y_pack")
    order = [(k, 2, k.ro) for k in colours] + [(k, s, q) for k in colours for s, q in ((0, k.rr), (1, k.rl))]
    for k in colours:
        k.sums = {}
    for k, s, q in order:
        accumulate(k.c, 4, 4, q)
        send_sums(k, s, q, 0)
    phase("y_packq")
    for k, s, q in order:
        send_sums(k, s, q, 1)
    phase("y_own")
    for k in colours:
        accumulate(k.c, 2, 6, k.r)

    def unpack(k, s, h):
        for b in range(HROWS // LANES):
            step = to_col(yauxr[k.c, s, h, b, 0:1, :], lane_eye(LANES))
            for j in range(LANES // OWN):
                high, low = decode(yrecv[k.c, s, h, b * (LANES // OWN) + j], step[j * OWN : (j + 1) * OWN])
                base = b * LANES + j * OWN
                acc[k.c, k.r, h, pl.ds(base, PAIRS), :] += high
                acc[k.c, k.r, h, pl.ds(base + PAIRS, PAIRS), :] += low

    zcopies = {}

    def z_send(h):
        phase(f"y_unpack{h}")
        for s in (0, 1, 2):
            for k in colours:
                arrive(k.sums[s, h])
                unpack(k, s, h)
        phase(f"z_pack{h}")
        for k in colours:
            def aux(b, step, count, k=k):
                zaux[h, b, 2 * k.c : 2 * k.c + 1, :] = step
                for s in range(3):
                    count = count + yauxr[k.c, s, h, b, 1:2, :]
                zaux[h, b, 2 * k.c + 1 : 2 * k.c + 2, :] = count

            pack(k.c, k.r, h, lambda zb, k=k: zsend.at[h, zb, k.c], aux)
        for d in (4, 3, 5, 2, 6, 1, 7):
            to = zat(d)
            zcopies[h, d] = [
                remote(zaux.at[h, to // (LANES // OWN)], zauxr.at[h, d - 1], at_z(to)),
                remote(zsend.at[h, to], zrecv.at[h, d - 1], at_z(to)),
            ]

    def own_to_slot(h, k, s, device):
        return [
            remote(ref.at[h, k.c, k.f, 0, z], ref.at[h, k.c, k.f, s, z], device) for ref in (words_ref, steps_ref)
        ]

    def z_sum(h):
        phase(f"z_sum{h}")
        mine = lane_eye(OWN, lax.rem(z, LANES // OWN) * OWN)
        for k in colours:
            sums = acc[k.c, k.r, h, pl.ds(pl.multiple_of(z * OWN, OWN), OWN), :]
            k.high, k.low = sums[:PAIRS], sums[PAIRS:]
            k.count = zaux[h, z // (LANES // OWN), 2 * k.c + 1 : 2 * k.c + 2, :]
        for d in (1, 7, 2, 6, 3, 5, 4):
            arrive(zcopies[h, d])
            for k in colours:
                step = to_col(zauxr[h, d - 1, 2 * k.c : 2 * k.c + 1, :], mine)
                high, low = decode(zrecv[h, d - 1, k.c], step)
                k.high, k.low = k.high + high, k.low + low
                k.count = k.count + zauxr[h, d - 1, 2 * k.c + 1 : 2 * k.c + 2, :]
        phase(f"fresh{h}")
        for k in colours:
            count = to_col(k.count, mine)
            rows = pl.ds(pl.multiple_of(k.r * CROWS + h * HROWS + z * OWN, OWN), OWN)
            prior = cv[0, rows, k.cols(k.f)].astype(jnp.float32)
            sums = jnp.concatenate([k.high, k.low], axis=0)
            code, step = encode(jnp.where(count > 0.5, sums / jnp.maximum(count, 1.0), prior))
            words_ref[h, k.c, k.f, 0, z] = pair(code)
            steps_ref[h, k.c, k.f, 0, z] = to_row(step, lane_eye(OWN))
            to_slots = ((2, k.ro), (3, k.rr), (1, k.rl))
            k.start[h] = sum((own_to_slot(h, k, s, k.at_r(to)) for s, to in to_slots), [])
        for k in colours if h == 0 else ():
            for way in (1, -1):
                to_slots = ((2, k.ro), (3, k.rr), (1, k.rl), (0, k.r))
                k.hops[h, way, 1] = sum((own_to_slot(h, k, s, k.at_rz(to, zat(way))) for s, to in to_slots), [])

    def group(h, k, f, zc, device):
        copies = []
        for ref in (words_ref, steps_ref):
            piece = ref.at[h, k.c, f, :, zc]
            copies.append(remote(piece, piece, device))
        return copies

    def hop(h, k, way, n):
        k.hops[h, way, n] = group(h, k, k.f, zat(-way * (n - 1)), at_z(zat(way)))

    def spread(h, k, d):
        targets = (k.fr, k.fl, k.fo) if (h, d) in STRAIGHT else (k.fr, k.fl)
        k.side[h, d] = [group(h, k, k.f, zat(d), k.at_f(to)) for to in targets]

    def relayed(h, ds):
        return [d for d in ds if (h, d) not in STRAIGHT]

    def left_first(d):
        return d in (0, 1, 2, 3)

    def across(h, *ds):
        phase(f"g_x{h}")
        for d in relayed(h, ds):
            for k in colours:
                from_left, from_right = k.side[h, d]
                if left_first(d):
                    arrive(from_left)
                    k.last[h, d] = group(h, k, k.fl, zat(d), k.at_f(k.fr)) + from_right
                else:
                    arrive(from_right)
                    k.last[h, d] = group(h, k, k.fr, zat(d), k.at_f(k.fl)) + from_left

    def finish(groups):
        def block(s, carry):
            for h, k, f, d in groups:
                zc = zat(d)
                step = to_col(steps_ref[h, k.c, f, s, zc], lane_eye(OWN))
                high, low = decode(words_ref[h, k.c, f, s, zc], step)
                base = pl.multiple_of(lax.rem(k.r + s, N) * CROWS + h * HROWS + zc * OWN, OWN)
                out_ref[pl.ds(base, PAIRS), k.cols(f)] = high
                out_ref[pl.ds(base + PAIRS, PAIRS), k.cols(f)] = low
            return carry

        lax.fori_loop(0, N, block, 0)

    def own_done(h, *ds):
        return [(h, k, k.f, d) for k in colours for d in ds]

    def first_done(h, *ds):
        return [(h, k, k.fl if left_first(d) else k.fr, d) for k in colours for d in relayed(h, ds)]

    def last_done(h, *ds):
        groups = []
        for k in colours:
            for d in ds:
                if (h, d) in STRAIGHT:
                    arrive(sum(k.side[h, d], []))
                    groups += [(h, k, f, d) for f in (k.fl, k.fr, k.fo)]
                else:
                    arrive(k.last[h, d])
                    groups += [(h, k, f, d) for f in (k.fo, k.fr if left_first(d) else k.fl)]
        return groups

    def sides_done(h, *ds):
        for k in colours:
            for d in ds:
                arrive(sum(k.side[h, d], []))
        return [(h, k, f, d) for k in colours for d in ds for f in (k.fl, k.fr)]

    def opposite_hop(h):
        for k in colours:
            k.opposite[h] = sum((group(h, k, k.fo, z, at_z(zat(way))) for way in (1, -1)), [])

    def opposite_done(h):
        for k in colours:
            arrive(k.opposite[h])
        return [(h, k, k.fo, d) for k in colours for d in (-1, 1)]

    def far_way(k):
        return 1 - 2 * k.c

    def gather_rows(h):
        phase(f"g_r{h}")
        for k in colours:
            arrive(k.start[h])
            if h == 1:
                hop(h, k, 1, 1)
                hop(h, k, -1, 1)
            spread(h, k, 0)

    def z_round(h, n):
        phase(f"g_z{n}h{h}")
        for k in colours:
            for way in (1, -1):
                if n < 4 or way == far_way(k):
                    arrive(k.hops[h, way, n])
                    if n < 3 or (n == 3 and way == far_way(k)):
                        hop(h, k, way, n + 1)
            for d in (-n, n) if n < 4 else (4,):
                spread(h, k, d)

    for k in colours:
        k.hops, k.side, k.start, k.last, k.opposite = {}, {}, {}, {}, {}
    z_send(0)
    phase("dist1a")
    c_p.wait_recv()
    distances(1, 0, 4)
    z_send(1)
    phase("dist1b")
    distances(1, 4, 2)
    early = list(used)
    z_sum(0)
    phase("dist1c")
    distances(1, 6, 2)
    eye = lane_eye(LANES)
    for b in range(ROWS // LANES):
        part = pv[pl.ds(b * LANES, LANES), :].astype(jnp.float32)
        square = to_row(jnp.sum(part * part, axis=1, keepdims=True), eye)
        lanes = pl.ds(b * LANES, LANES)
        cost_ref[:, lanes] = (square + jnp.min(best[:, lanes], axis=0, keepdims=True)) * (1.0 / 1024)
    z_sum(1)
    for copy in early:
        copy.wait_send()
    gather_rows(0)
    z_round(0, 1)
    gather_rows(1)
    across(0, 0)
    phase("g_f0")
    finish(own_done(0, 0, -1, 1) + first_done(0, 0))
    z_round(0, 2)
    z_round(1, 1)
    across(1, 0)
    phase("g_f1")
    done = last_done(0, 0)
    opposite_hop(0)
    finish(own_done(0, -2, 2) + own_done(1, 0) + done)
    z_round(0, 3)
    z_round(1, 2)
    across(0, -2, 2)
    phase("g_f2")
    done = last_done(1, 0)
    opposite_hop(1)
    finish(own_done(0, -3, 3) + own_done(1, -1, 1) + first_done(0, -2, 2) + first_done(1, 0) + sides_done(0, -1, 1) + done)
    z_round(0, 4)
    z_round(1, 3)
    across(0, -3, 3)
    across(1, -2, 2)
    phase("g_f3")
    finish(own_done(0, 4) + own_done(1, -2, 2) + opposite_done(0))
    z_round(1, 4)
    across(0, 4)
    across(1, -3, 3)
    phase("g_f4")
    finish(own_done(1, -3, 3, 4) + first_done(0, -3, 3) + first_done(1, -2, 2) + last_done(0, -2, 2) + sides_done(1, -1, 1))
    across(1, 4)
    phase("g_f5")
    finish(first_done(0, 4) + first_done(1, -3, 3, 4) + last_done(0, -3, 3) + opposite_done(1))
    phase("g_f6")
    finish(last_done(0, 4) + last_done(1, -2, 2))
    phase("g_f7")
    finish(last_done(1, -3, 3))
    for copy in used[len(early) : -24]:
        copy.wait_send()
    phase("g_f8")
    finish(last_done(1, 4))
    phase("w_send")
    for copy in used[-24:]:
        copy.wait_send()
    phase(None)
    assert len(used) == N_COPIES, len(used)


N_COPIES = 382
STRAIGHT = ((1, 4), (1, 3), (1, -3), (0, 4), (0, 3), (0, -3))


def put_kernel(rows_ref, cost_ref, rows_hbm, cost_hbm, sems):
    puts = [pltpu.make_async_copy(cost_ref, cost_hbm, sems.at[N])]
    for q in range(N):
        rows = pl.ds(q * CROWS, CROWS)
        puts.append(pltpu.make_async_copy(rows_ref.at[rows], rows_hbm.at[rows], sems.at[q]))
    for put in puts:
        put.start()
    for put in puts:
        put.wait()


def shards(points, centroids, assign, keep_mask):
    vmem = pl.BlockSpec(memory_space=pltpu.VMEM)
    hbm = pl.BlockSpec(memory_space=pltpu.HBM)
    dma = pltpu.SemaphoreType.DMA
    f32, i32, bf16 = jnp.float32, jnp.int32, jnp.bfloat16
    args = (points, centroids, assign.reshape(1, ROWS), keep_mask.reshape(1, ROWS))
    rows, cost = pl.pallas_call(
        update_kernel,
        out_shape=(
            jax.ShapeDtypeStruct((2048, 1024), f32),
            jax.ShapeDtypeStruct((1, ROWS), f32),
        ),
        in_specs=[hbm] * 4,
        out_specs=(vmem, vmem),
        scratch_shapes=[
            pltpu.VMEM((2, 2, N, N, NZ, PAIRS, LANES), i32),
            pltpu.VMEM((2, 2, N, N, NZ, 1, LANES), f32),
            pltpu.VMEM((ROWS, 1024), bf16),
            pltpu.VMEM((2, 2048, 1024), bf16),
            pltpu.VMEM((2, 1, ROWS), i32),
            pltpu.VMEM((2 * ROWS, 2 * LANES), bf16),
            pltpu.VMEM((2, 6 * ROWS, LANES), bf16),
            pltpu.VMEM((1, 2 * ROWS), i32),
            pltpu.VMEM((2, 1, 6 * ROWS), i32),
            pltpu.VMEM((2, 2, ROWS // 2, LANES), bf16),
            pltpu.VMEM((8, ROWS), f32),
            pltpu.VMEM((2, N, 2, HROWS, LANES), f32),
            pltpu.VMEM((2, N, 2, HROWS, LANES), bf16),
            pltpu.VMEM((2, 3, 2, NZ, PAIRS, LANES), i32),
            pltpu.VMEM((2, 3, 2, 2, 2, LANES), f32),
            pltpu.VMEM((2, 3, 2, NZ, PAIRS, LANES), i32),
            pltpu.VMEM((2, 3, 2, 2, 2, LANES), f32),
            pltpu.VMEM((2, NZ, 2, PAIRS, LANES), i32),
            pltpu.VMEM((2, 2, 4, LANES), f32),
            pltpu.VMEM((2, NZ - 1, 2, PAIRS, LANES), i32),
            pltpu.VMEM((2, NZ - 1, 4, LANES), f32),
            dma((N_COPIES,)), dma((N_COPIES,)), dma((6,)),
        ],
        compiler_params=pltpu.CompilerParams(
            collective_id=0, has_side_effects=True, vmem_limit_bytes=40 * 1024 * 1024
        ),
    )(*(pltpu.with_memory_space_constraint(a, pltpu.HBM) for a in args))
    new_centroids, cost = pl.pallas_call(
        put_kernel,
        out_shape=(jax.ShapeDtypeStruct((2048, 1024), f32), jax.ShapeDtypeStruct((1, ROWS), f32)),
        in_specs=[vmem] * 2,
        out_specs=(hbm, hbm),
        scratch_shapes=[dma((N + 1,))],
        compiler_params=pltpu.CompilerParams(vmem_limit_bytes=1024 * 1024),
        cost_estimate=pl.CostEstimate(flops=0, bytes_accessed=16 << 20, transcendentals=0),
    )(rows, cost)
    return new_centroids, cost.reshape(ROWS)


def solution(mesh):
    grid = Mesh(mesh.devices.reshape(NZ, N, N, 2), ("z", "y", "x", "mp"))
    rows = ("z", "y", "x", "mp")
    in_specs = (P(rows, None), P("mp", None), P(rows), P(rows))
    out_specs = (P("mp", None), P(rows))
    return jax.shard_map(shards, mesh=grid, in_specs=in_specs, out_specs=out_specs, check_vma=False)
```
